32 devices in a mesh: tm: 16 (over z, y, core), space: 2 (over x).
Axes of the slice: x: 2, y: 2, z: 4, core: 2. Of those that a mesh axis runs over, the one named last changes fastest.
Arguments:
- iterate: float32 [16, 4, 128, 64, 128], P('tm', None, 'space'), may hold values from -6 to 6
- right_side: float32 [16, 4, 128, 64, 128], P('tm', None, 'space'), may hold values from -6 to 6
- diffusivity: float32 [128, 64, 128], P('space'), may hold values from 0.5 to 2
- velocity: float32 [3], replicated, may hold values from -2 to 2
Outputs:
- next_iterate: float32 [16, 4, 128, 64, 128], P('tm', None, 'space')
The draws below stay inside these ranges and needn't reach their ends.
All inputs are finite; a program needn't handle non-finite values.
Results may differ from the reference program's by a relative error of at most 0.0003.
Values sent between devices are 32-bit elements; how exact they have to be, the bound alone decides.
A program may use at most 192 MiB of HBM per device.

```python
import math
import jax
import jax.numpy as jnp
from jax import lax

NX = 128
NY = 128
NZ = 64
NODES = 4
STEPS = 16


def draw_right_side(key, part):
    rough_key = jax.random.fold_in(jax.random.fold_in(key, 17), 0)
    rough = jax.random.truncated_normal(rough_key, -6.0, 6.0, (STEPS, NODES, NX, NZ, NY), jnp.float32)
    return rough


def block_levels(key, extent, pieces, least, largest):
    def one(axis_at, shards_of):
        steps = jax.random.uniform(jax.random.fold_in(jax.random.fold_in(key, 6), axis_at), (shards_of,), jnp.float32, least / len(pieces), largest / len(pieces))
        return jnp.repeat(jnp.exp(steps), extent[axis_at] // shards_of).reshape((-1,) + (1,) * (len(extent) - axis_at - 1))

    factor_of = one(*pieces[0])
    for cut in pieces[1:]:
        factor_of = factor_of * one(*cut)
    return factor_of


def centred(own_key, shape, spread, limit, pieces=(), kind=jnp.bfloat16):
    level = block_levels(own_key, shape, pieces, -0.22, 0.18) if pieces else 1.0
    values = jax.random.normal(own_key, shape, jnp.float32) * spread * level
    return jnp.minimum(jnp.maximum(values, -limit), limit).astype(kind)


def setup_inputs(seed: int = 0) -> dict:
    streams_of = jax.random.split(jax.random.key(seed), 5)
    return {
        "iterate": centred(streams_of[0], (STEPS, NODES, NX, NZ, NY), 1.0, 6.0, ((0, 16), (2, 2)), jnp.float32),
        "right_side": draw_right_side(jax.random.fold_in(streams_of[4], 71), 0),
        "diffusivity": jnp.clip(jnp.exp(math.log(2.0) - 1.3862944 * jax.random.uniform(streams_of[2], (NX, NZ, NY), jnp.float32) ** block_levels(streams_of[2], (NX, NZ, NY), ((0, 2),), -0.2, 0.2)), 0.5, 2.0),
        "velocity": jnp.clip(jax.random.uniform(streams_of[3], (3,), jnp.float32, -2.0, 2.0), -2.0, 2.0),
    }


diffusion_number = 16.0
circulant_alpha = 0.1


def collocation_matrix():
    radau_nodes = [0.088587959512703947, 0.40946686444073471, 0.78765946176084706, 1.0]
    matrix = [[0.0] * 4 for row_index in range(4)]
    for column_index in range(4):
        coefficients = [1.0]
        for other_index in range(4):
            if other_index != column_index:
                scale_value = 1.0 / (radau_nodes[column_index] - radau_nodes[other_index])
                shifted = [0.0] + [value * scale_value for value in coefficients]
                lowered = [-radau_nodes[other_index] * scale_value * value for value in coefficients] + [0.0]
                coefficients = [left_value + right_value for left_value, right_value in zip(shifted, lowered)]
        for row_index in range(4):
            total = 0.0
            for power_index in range(len(coefficients)):
                total = total + coefficients[power_index] * radau_nodes[row_index] ** (power_index + 1) / (power_index + 1)
            matrix[row_index][column_index] = total
    return matrix


def solve_system(matrix, target):
    count = len(target)
    rows_list = [list(matrix[row_index]) + [target[row_index]] for row_index in range(count)]
    for column in range(count):
        best_row = column
        for candidate in range(column + 1, count):
            if abs(rows_list[candidate][column]) > abs(rows_list[best_row][column]):
                best_row = candidate
        saved_row = rows_list[column]
        rows_list[column] = rows_list[best_row]
        rows_list[best_row] = saved_row
        leader = rows_list[column][column]
        for other_row in range(count):
            if other_row != column:
                factor = rows_list[other_row][column] / leader
                rows_list[other_row] = [left_value - factor * right_value for left_value, right_value in zip(rows_list[other_row], rows_list[column])]
    return [rows_list[row_index][count] / rows_list[row_index][row_index] for row_index in range(count)]


def node_basis():
    matrix = collocation_matrix()
    helper = [[0.0] * 4 for row_index in range(4)]
    coefficients = [0.0, 0.0, 0.0, 0.0, 1.0]
    for order in range(1, 5):
        product = [[sum(matrix[row_index][inner] * helper[inner][column] for inner in range(4)) for column in range(4)] for row_index in range(4)]
        for row_index in range(4):
            product[row_index][row_index] = product[row_index][row_index] + coefficients[5 - order]
        helper = product
        trace_value = sum(sum(matrix[row_index][inner] * helper[inner][row_index] for inner in range(4)) for row_index in range(4))
        coefficients[4 - order] = -trace_value / order
    roots_list = [(0.4 + 0.9j) ** power_index for power_index in range(4)]
    for sweep in range(400):
        for root_index in range(4):
            current = roots_list[root_index]
            numer = 0.0
            for power_index in range(4, -1, -1):
                numer = numer * current + coefficients[power_index]
            denom = 1.0
            for other_index in range(4):
                if other_index != root_index:
                    denom = denom * (current - roots_list[other_index])
            roots_list[root_index] = current - numer / denom
    vectors = [[0.0] * 4 for row_index in range(4)]
    for root_index in range(4):
        shifted = [[matrix[row_index][column] - (roots_list[root_index] if row_index == column else 0.0) for column in range(3)] for row_index in range(3)]
        target = [-matrix[row_index][3] for row_index in range(3)]
        parts = solve_system(shifted, target) + [1.0 + 0.0j]
        for row_index in range(4):
            vectors[row_index][root_index] = parts[row_index]
    inverse = [[0.0] * 4 for row_index in range(4)]
    for column in range(4):
        unit = [1.0 if row_index == column else 0.0 for row_index in range(4)]
        parts = solve_system(vectors, unit)
        for row_index in range(4):
            inverse[row_index][column] = parts[row_index]
    weights = [sum(inverse[row_index][column] for column in range(4)) for row_index in range(4)]
    return roots_list, vectors, inverse, weights


def complex_vector(numbers):
    real_values = jnp.asarray([complex(value).real for value in numbers], jnp.float32)
    imag_values = jnp.asarray([complex(value).imag for value in numbers], jnp.float32)
    return real_values + 1j * imag_values


def complex_matrix(numbers):
    real_values = jnp.asarray([[complex(value).real for value in row] for row in numbers], jnp.float32)
    imag_values = jnp.asarray([[complex(value).imag for value in row] for row in numbers], jnp.float32)
    return real_values + 1j * imag_values


def spatial_operator(field_values, diffusivity, velocity):
    upper_x = jnp.roll(field_values, -1, axis=2)
    lower_x = jnp.roll(field_values, 1, axis=2)
    upper_z = jnp.roll(field_values, -1, axis=3)
    lower_z = jnp.roll(field_values, 1, axis=3)
    upper_y = jnp.roll(field_values, -1, axis=4)
    lower_y = jnp.roll(field_values, 1, axis=4)
    laplace = (upper_x + lower_x) + (upper_z + lower_z) + (upper_y + lower_y) - 6.0 * field_values
    transport = velocity[0] * (upper_x - lower_x) + velocity[1] * (upper_y - lower_y) + velocity[2] * (upper_z - lower_z)
    return diffusion_number * diffusivity * laplace - 0.5 * transport


def reference(iterate, right_side, diffusivity, velocity):
    collocation = jnp.asarray(collocation_matrix(), jnp.float32)
    applied = spatial_operator(iterate, diffusivity, velocity)
    coupled = jnp.einsum("mn,snxzy->smxzy", collocation, applied, precision=lax.Precision.HIGHEST)
    previous = jnp.concatenate([jnp.zeros_like(iterate[:1, 3]), iterate[:-1, 3]], axis=0)
    residual = right_side - iterate + coupled + previous[:, None]
    gamma_base = circulant_alpha ** (1.0 / STEPS)
    step_power = jnp.arange(STEPS, dtype=jnp.int32).astype(jnp.float32)
    step_scale = jnp.power(jnp.float32(gamma_base), step_power)
    spectrum = jnp.fft.rfftn(residual * step_scale[:, None, None, None, None], axes=(0, 2, 3, 4))
    theta_x = jnp.arange(NX, dtype=jnp.int32).astype(jnp.float32) * (2.0 * math.pi / NX)
    theta_z = jnp.arange(NZ, dtype=jnp.int32).astype(jnp.float32) * (2.0 * math.pi / NZ)
    theta_y = jnp.arange(NY // 2 + 1, dtype=jnp.int32).astype(jnp.float32) * (2.0 * math.pi / NY)
    symbol_real = diffusion_number * ((2.0 * jnp.cos(theta_x)[:, None, None] - 2.0) + (2.0 * jnp.cos(theta_z)[None, :, None] - 2.0) + (2.0 * jnp.cos(theta_y)[None, None, :] - 2.0))
    symbol_imag = -(velocity[0] * jnp.sin(theta_x)[:, None, None] + velocity[1] * jnp.sin(theta_y)[None, None, :] + velocity[2] * jnp.sin(theta_z)[None, :, None])
    symbol = symbol_real + 1j * symbol_imag
    values, vectors, inverse, weights = node_basis()
    eigen = complex_vector(values)
    basis = complex_matrix(vectors)
    basis_inverse = complex_matrix(inverse)
    ones_weights = complex_vector(weights)
    damping = 1.0 / (1.0 - eigen[:, None, None, None] * symbol[None])
    ones_image = jnp.einsum("pm,mxzy->pxzy", basis, ones_weights[:, None, None, None] * damping, precision=lax.Precision.HIGHEST)
    phases = jnp.arange(STEPS, dtype=jnp.int32).astype(jnp.float32) * (2.0 * math.pi / STEPS)
    shift_factors = gamma_base * (jnp.cos(phases) - 1j * jnp.sin(phases))

    def solve_one(operands):
        block, shift_factor = operands
        inner = jnp.einsum("mn,nxzy->mxzy", basis_inverse, block, precision=lax.Precision.HIGHEST) * damping
        image = jnp.einsum("pm,mxzy->pxzy", basis, inner, precision=lax.Precision.HIGHEST)
        factor = shift_factor * image[3] / (1.0 - shift_factor * ones_image[3])
        return image + ones_image * factor[None]

    solved = lax.map(solve_one, (spectrum, shift_factors))
    correction = jnp.fft.irfftn(solved, s=(STEPS, NX, NZ, NY), axes=(0, 2, 3, 4))
    unscale = jnp.power(jnp.float32(gamma_base), -step_power)
    return iterate + correction * unscale[:, None, None, None, None]
```

```python
import functools
import math

import jax
import jax.numpy as jnp
import numpy as np
from jax import lax
from jax.experimental import pallas as pl
from jax.experimental.pallas import tpu as pltpu
from jax.sharding import PartitionSpec as P

diffusion_number = 16.0
circulant_alpha = 0.1


def collocation_matrix():
    radau_nodes = [0.08858795951270394, 0.4094668644407347, 0.7876594617608471, 1.0]
    matrix = [[0.0] * 4 for row_index in range(4)]
    for column_index in range(4):
        coefficients = [1.0]
        for other_index in range(4):
            if other_index != column_index:
                scale_value = 1.0 / (radau_nodes[column_index] - radau_nodes[other_index])
                shifted = [0.0] + [value * scale_value for value in coefficients]
                lowered = [
                    -radau_nodes[other_index] * scale_value * value for value in coefficients
                ] + [0.0]
                coefficients = [
                    left_value + right_value for left_value, right_value in zip(shifted, lowered)
                ]
        for row_index in range(4):
            total = 0.0
            for power_index in range(len(coefficients)):
                total = total + coefficients[power_index] * radau_nodes[row_index] ** (
                    power_index + 1
                ) / (power_index + 1)
            matrix[row_index][column_index] = total
    return matrix


def solve_system(matrix, target):
    count = len(target)
    rows_list = [list(matrix[row_index]) + [target[row_index]] for row_index in range(count)]
    for column in range(count):
        best_row = column
        for candidate in range(column + 1, count):
            if abs(rows_list[candidate][column]) > abs(rows_list[best_row][column]):
                best_row = candidate
        saved_row = rows_list[column]
        rows_list[column] = rows_list[best_row]
        rows_list[best_row] = saved_row
        leader = rows_list[column][column]
        for other_row in range(count):
            if other_row != column:
                factor = rows_list[other_row][column] / leader
                rows_list[other_row] = [
                    left_value - factor * right_value
                    for left_value, right_value in zip(rows_list[other_row], rows_list[column])
                ]
    return [
        rows_list[row_index][count] / rows_list[row_index][row_index] for row_index in range(count)
    ]


def node_basis():
    matrix = collocation_matrix()
    helper = [[0.0] * 4 for row_index in range(4)]
    coefficients = [0.0, 0.0, 0.0, 0.0, 1.0]
    for order in range(1, 5):
        product = [
            [
                sum((matrix[row_index][inner] * helper[inner][column] for inner in range(4)))
                for column in range(4)
            ]
            for row_index in range(4)
        ]
        for row_index in range(4):
            product[row_index][row_index] = product[row_index][row_index] + coefficients[5 - order]
        helper = product
        trace_value = sum(
            (
                sum((matrix[row_index][inner] * helper[inner][row_index] for inner in range(4)))
                for row_index in range(4)
            )
        )
        coefficients[4 - order] = -trace_value / order
    roots_list = [(0.4 + 0.9j) ** power_index for power_index in range(4)]
    for sweep in range(400):
        for root_index in range(4):
            current = roots_list[root_index]
            numer = 0.0
            for power_index in range(4, -1, -1):
                numer = numer * current + coefficients[power_index]
            denom = 1.0
            for other_index in range(4):
                if other_index != root_index:
                    denom = denom * (current - roots_list[other_index])
            roots_list[root_index] = current - numer / denom
    vectors = [[0.0] * 4 for row_index in range(4)]
    for root_index in range(4):
        shifted = [
            [
                matrix[row_index][column] - (roots_list[root_index] if row_index == column else 0.0)
                for column in range(3)
            ]
            for row_index in range(3)
        ]
        target = [-matrix[row_index][3] for row_index in range(3)]
        parts = solve_system(shifted, target) + [1.0 + 0j]
        for row_index in range(4):
            vectors[row_index][root_index] = parts[row_index]
    inverse = [[0.0] * 4 for row_index in range(4)]
    for column in range(4):
        unit = [1.0 if row_index == column else 0.0 for row_index in range(4)]
        parts = solve_system(vectors, unit)
        for row_index in range(4):
            inverse[row_index][column] = parts[row_index]
    weights = [sum((inverse[row_index][column] for column in range(4))) for row_index in range(4)]
    return (roots_list, vectors, inverse, weights)


def split_constant(matrix):
    high = matrix.astype(jnp.bfloat16)
    low = (matrix - high.astype(np.float64)).astype(jnp.bfloat16)
    return high, low


def split(value):
    high = value.astype(jnp.bfloat16)
    low = (value - high.astype(jnp.float32)).astype(jnp.bfloat16)
    return high, low


def dot(left, right):
    return jnp.dot(left, right, preferred_element_type=jnp.float32)


def table_times(high, low, value):
    value_high, value_low = split(value)
    return dot(high, value_high) + dot(high, value_low) + dot(low, value_high)


def times_table(value, high, low):
    value_high, value_low = split(value)
    return dot(value_high, high) + dot(value_low, high) + dot(value_high, low)


def tripled(value):
    high = value.astype(jnp.bfloat16).astype(jnp.float32)
    return jnp.concatenate((high, value - high, high), axis=0).astype(jnp.bfloat16)


def tripled_constant(matrix):
    high, low = split_constant(matrix)
    return np.concatenate((high, high, low), axis=1)


def complex_block(matrix):
    return np.block([[matrix.real, -matrix.imag], [matrix.imag, matrix.real]])


def fourier(rows, columns, length, sign):
    phases = np.outer(rows, columns) % length
    return np.exp(sign * 2j * np.pi * phases / length)


class Plan:
    def __init__(self, slabs, steps, size_x, size_z, size_y):
        self.slabs, self.steps = slabs, steps
        self.size_x, self.size_z, self.size_y = size_x, size_z, size_y
        self.long = long = size_x // slabs
        self.planes = size_z // 2 + 1
        each = -(-self.planes // slabs)
        while (each * slabs) % 2:
            each += 1
        self.each = each
        self.padded = each * slabs
        self.rows = 4 * self.padded
        self.block = 8
        self.blocks = long // self.block
        self.own_x = size_x // steps
        self.sent = 2 * long + 16
        self.values, self.vectors, self.inverse, self.weights = node_basis()
        self.matrix = np.array(collocation_matrix())

    def symbol_tables(self, length):
        theta_x = 2.0 * np.pi * np.arange(length)[:, None] / length
        theta_y = 2.0 * np.pi * np.arange(self.size_y)[None, :] / self.size_y
        real = diffusion_number * (2.0 * np.cos(theta_x) + 2.0 * np.cos(theta_y) - 4.0)
        ones = np.ones_like(real)
        return np.stack((real, np.sin(theta_x) * ones, np.sin(theta_y) * ones)).astype(np.float32)

    def z_symbols(self):
        theta = 2.0 * np.pi * np.arange(self.padded) / self.size_z
        return np.stack((diffusion_number * (2.0 * np.cos(theta) - 2.0), np.sin(theta))).astype(
            np.float32
        )

    def z_forward(self):
        wave = fourier(np.arange(self.padded), np.arange(self.size_z), self.size_z, -1.0)
        wave[self.planes :] = 0.0
        full = np.einsum("mn,kz->mknz", np.array(self.inverse), wave)
        full = full.reshape(self.rows, 4 * self.size_z)
        return np.concatenate((full.real, full.imag), axis=0)

    def z_backward(self):
        wave = fourier(np.arange(self.size_z), np.arange(self.padded), self.size_z, 1.0)
        weight = np.full(self.padded, 2.0)
        weight[0] = 1.0
        weight[self.planes - 1] = 1.0
        weight[self.planes :] = 0.0
        wave = wave * weight / self.size_z
        full = np.einsum("nm,zk->nzmk", np.array(self.vectors), wave)
        full = full.reshape(4 * self.size_z, self.rows)
        return np.concatenate((full.real, -full.imag), axis=1)

    def y_forward(self):
        span = np.arange(self.size_y)
        return complex_block(fourier(span, span, self.size_y, -1.0)).T

    def y_backward(self):
        span = np.arange(self.size_y)
        return complex_block(fourier(span, span, self.size_y, 1.0)).T / self.size_y

    def x_forward(self, length):
        span = np.arange(length)
        return complex_block(fourier(span, span, length, -1.0))

    def x_backward(self, length):
        span = np.arange(length)
        return complex_block(fourier(span, span, length, 1.0)) / length

    def ends(self):
        points = np.array([0, self.long - 1])
        wave = fourier(points, np.arange(self.long), self.long, 1.0) / self.long
        full = complex_block(wave)[[0, 2, 1, 3]]
        return np.concatenate((full, full, full, full), axis=0)

    def jump_sources(self):
        wave = np.arange(self.size_x)
        even = []
        for slab in range(self.slabs):
            start = slab * self.long

            def phase(point):
                return fourier(wave, np.array([point % self.size_x]), self.size_x, -1.0)[:, 0]

            first = phase(start - 1) - phase(start + self.long - 1)
            last = phase(start + self.long) - phase(start)
            even.append(np.stack((first, 1j * first, last, 1j * last), axis=1))
        return self.by_parity(even)

    def by_parity(self, blocks):
        zero = np.zeros_like(blocks[0])
        even = np.concatenate([part for block in blocks for part in (block, zero)], axis=1)
        odd = np.concatenate([part for block in blocks for part in (zero, block)], axis=1)
        return [np.concatenate((full.real, full.imag), axis=0) for full in (even, odd)]

    def end_sources(self):
        wave = np.arange(self.long)
        upper = fourier(wave, np.array([1]), self.long, 1.0)[:, 0]
        lower = np.ones_like(upper)
        return self.by_parity([np.stack((upper, 1j * upper, lower, 1j * lower), axis=1)])

    def jumps(self):
        wave = np.arange(self.size_x)
        rows = []
        for slab in range(self.slabs):
            start = slab * self.long
            points = np.array([start + self.long, start, start - 1, start + self.long - 1])
            value = fourier(points % self.size_x, wave, self.size_x, 1.0) / self.size_x
            upper, lower = value[0] - value[1], value[2] - value[3]
            full = complex_block(np.stack((upper, lower)))[[0, 2, 1, 3]]
            rows += [full, full]
        return np.concatenate(rows, axis=0)


def damped_by(real, imag, value):
    lower_real = 1.0 - (real * value.real - imag * value.imag)
    lower_imag = real * value.imag + imag * value.real
    scale = 1.0 / (lower_real * lower_real + lower_imag * lower_imag)
    return lower_real * scale, lower_imag * scale


def symbol(table, floats, wave_z, plane):
    real = table[0] + wave_z[0, plane]
    imag = -(floats[0] * table[1] + floats[1] * table[2] + floats[2] * wave_z[1, plane])
    return real, imag


def times(left, right):
    return (left[0] * right[0] - left[1] * right[1], left[0] * right[1] + left[1] * right[0])


def plus(left, right):
    return (left[0] + right[0], left[1] + right[1])


def number(value):
    value = complex(value)
    return (value.real, value.imag)


def end_scale(floats, shape):
    row = lax.broadcasted_iota(jnp.int32, shape, 0) % 4
    upper = diffusion_number - 0.5 * floats[0]
    lower = diffusion_number + 0.5 * floats[0]
    return jnp.where(row < 2, upper, lower)


def enter_kernel(plan, floats, it, below, above, low_halo, high_halo, right, diff, *refs):
    z_high, z_low, y_high, y_low, out_real, out_imag, buffer = refs
    block, rows, size_y = plan.block, plan.rows, plan.size_y
    at = pl.program_id(0)
    first, last = at == 0, at == pl.num_programs(0) - 1
    buffer[:, 1 : block + 1] = it[...]
    buffer[:, 0:1] = jnp.where(first, low_halo[...], below[...])
    buffer[:, block + 1 :] = jnp.where(last, high_halo[...], above[...])
    nodes = plan.matrix.sum(axis=1)
    size_z = plan.size_z

    def driving(plane):
        factor = diffusion_number * (diff[plane] - 1.0)
        terms = []
        for node in range(4):
            center = buffer[node, plane + 1]
            upper, lower = buffer[node, plane + 2], buffer[node, plane]
            z_up, z_down = pltpu.roll(center, size_z - 1, 0), pltpu.roll(center, 1, 0)
            y_up, y_down = pltpu.roll(center, size_y - 1, 1), pltpu.roll(center, 1, 1)
            laplace = (upper + lower) + (z_up + z_down) + (y_up + y_down) - 6.0 * center
            terms.append(factor * laplace)
        transport = (
            floats[0] * (upper - lower) + floats[1] * (y_up - y_down) + floats[2] * (z_up - z_down)
        )
        operated = floats[3] * (diffusion_number * laplace - 0.5 * transport)
        kept = floats[3] * center
        result = []
        for row in range(4):
            total = right[row, plane] + (float(nodes[row]) * operated - kept)
            for column in range(4):
                total = total + float(plan.matrix[row, column]) * terms[column]
            result.append(total)
        return jnp.concatenate(result, axis=0)

    def pair(index, carry):
        plane = 2 * index
        both = jnp.concatenate((driving(plane), driving(plane + 1)), axis=1)
        along_z = table_times(z_high[...], z_low[...], both)
        real, imag = along_z[:rows], along_z[rows:]
        stacked = jnp.concatenate(
            (
                jnp.concatenate((real[:, :size_y], imag[:, :size_y]), axis=1),
                jnp.concatenate((real[:, size_y:], imag[:, size_y:]), axis=1),
            ),
            axis=0,
        )
        along_y = times_table(stacked, y_high[...], y_low[...])
        for offset in range(2):
            part = along_y[offset * rows : (offset + 1) * rows]
            where = pl.ds(plane + offset, rows, stride=block)
            out_real[0, where, :] = part[:, :size_y]
            out_imag[0, where, :] = part[:, size_y:]
        return carry

    lax.fori_loop(0, block // 2, pair, 0)


def modes_kernel(plan, floats, wave_z, in_real, in_imag, table, *refs):
    f_high, f_low, b_high, b_low, e_high, e_low, out_real, out_imag, sent = refs
    long, size_y = plan.long, plan.size_y
    plane = pl.program_id(0)
    real = [in_real[:, mode, 0].reshape(long, size_y) for mode in range(4)]
    imag = [in_imag[:, mode, 0].reshape(long, size_y) for mode in range(4)]
    value = jnp.concatenate(
        (jnp.concatenate(real, axis=1), jnp.concatenate(imag, axis=1)), axis=0
    )
    spectrum = table_times(f_high[...], f_low[...], value)
    a_real, a_imag = symbol(table, floats, wave_z, plane)
    total, inner = None, []
    for mode in range(4):
        lanes = slice(mode * size_y, (mode + 1) * size_y)
        part = (spectrum[:long, lanes], spectrum[long:, lanes])
        out_real[0, mode], out_imag[0, mode] = part
        part = times(damped_by(a_real, a_imag, complex(plan.values[mode])), part)
        total = part if total is None else plus(total, part)
        inner.append(jnp.concatenate(part, axis=0))
    last = table_times(b_high[...], b_low[...], jnp.concatenate(total, axis=0))
    sent[0, : 2 * long] = last
    ends = table_times(e_high[...], e_low[...], jnp.concatenate(inner, axis=1))[:8]
    upper = lax.broadcasted_iota(jnp.int32, (8, size_y), 0) < 4
    for pair in range(2):
        even = ends[:, 2 * pair * size_y : (2 * pair + 1) * size_y]
        odd = ends[:, (2 * pair + 1) * size_y : (2 * pair + 2) * size_y]
        start = 2 * long + 8 * pair
        sent[0, start : start + 8] = jnp.where(upper, even, odd)


def end_spectra(plan, floats, tiles, even, odd):
    size_x, size_y = plan.size_x, plan.size_y
    pairs = []
    for pair in range(2):
        rows = jnp.concatenate([tiles[slab][8 * pair : 8 * pair + 8] for slab in range(plan.slabs)])
        pairs.append(rows * end_scale(floats, rows.shape))
    value = tripled(jnp.concatenate(pairs, axis=1))
    found = [dot(even[...], value), dot(odd[...], value)]
    result = []
    for mode in range(4):
        lanes = slice((mode // 2) * size_y, (mode // 2 + 1) * size_y)
        part = found[mode % 2][:, lanes]
        result.append(times(number(plan.values[mode]), (part[:size_x], part[size_x:])))
    return result


def last_kernel(plan, floats, wave_z, places, arrived, table, f_high, f_low, even, odd, out):
    long, size_x = plan.long, plan.size_x
    plane = places[1] * plan.each + pl.program_id(0)
    slabs = range(plan.slabs)
    value = jnp.concatenate(
        [arrived[slab, 0, :long] for slab in slabs]
        + [arrived[slab, 0, long : 2 * long] for slab in slabs],
        axis=0,
    )
    found = table_times(f_high[...], f_low[...], value)
    total = (found[:size_x], found[size_x:])
    tiles = [arrived[slab, 0, 2 * long :] for slab in slabs]
    sources = end_spectra(plan, floats, tiles, even, odd)
    a_real, a_imag = symbol(table, floats, wave_z, plane)
    for mode in range(4):
        damped = damped_by(a_real, a_imag, complex(plan.values[mode]))
        total = plus(total, times(damped, sources[mode]))
    own = plan.own_x
    for step in range(plan.steps):
        rows = slice(step * own, (step + 1) * own)
        out[step, 0, :own] = total[0][rows]
        out[step, 0, own:] = total[1][rows]


def sweep_kernel(plan, floats, wave_z, places, arrived, table, out):
    own = plan.own_x
    plane = places[1] * plan.each + pl.program_id(0)
    rows = pl.ds(pl.multiple_of(places[0] * own, own), own)
    a_real, a_imag = symbol([table[index, rows] for index in range(3)], floats, wave_z, plane)
    growth = None
    for mode in range(4):
        damped = damped_by(a_real, a_imag, complex(plan.values[mode]))
        term = times(number(plan.weights[mode]), damped)
        growth = term if growth is None else plus(growth, term)
    fields = [(arrived[step, 0, :own], arrived[step, 0, own:]) for step in range(plan.steps)]
    total, power = fields[0], growth
    for step in range(1, plan.steps):
        total = plus(fields[step], times(growth, total))
        power = times(growth, power)
    lower = (1.0 - circulant_alpha * power[0], -circulant_alpha * power[1])
    scale = circulant_alpha / (lower[0] * lower[0] + lower[1] * lower[1])
    current = times(total, (lower[0] * scale, -lower[1] * scale))
    for step in range(plan.steps):
        out[step, 0, :own] = current[0]
        out[step, 0, own:] = current[1]
        current = plus(fields[step], times(growth, current))


def driven_kernel(plan, floats, wave_z, places, before, arrived, table, *refs):
    b_high, b_low, even, odd, j_high, j_low, out = refs
    long, size_x, size_y, own = plan.long, plan.size_x, plan.size_y, plan.own_x
    plane = places[1] * plan.each + pl.program_id(0)
    real = jnp.concatenate([before[step, 0, :own] for step in range(plan.steps)], axis=0)
    imag = jnp.concatenate([before[step, 0, own:] for step in range(plan.steps)], axis=0)
    found = table_times(b_high[...], b_low[...], jnp.concatenate((real, imag), axis=0))
    tiles = [arrived[slab, 0] for slab in range(plan.slabs)]
    sources = end_spectra(plan, floats, tiles, even, odd)
    a_real, a_imag = symbol(table, floats, wave_z, plane)
    driven = []
    for mode in range(4):
        damped = damped_by(a_real, a_imag, complex(plan.values[mode]))
        weighted = times(number(plan.weights[mode]), (real, imag))
        driven.append(jnp.concatenate(times(damped, plus(weighted, sources[mode])), axis=0))
    jumps = table_times(j_high[...], j_low[...], jnp.concatenate(driven, axis=1))
    row = lax.broadcasted_iota(jnp.int32, (8, size_y), 0)
    for slab in range(plan.slabs):
        out[slab, 0, :long] = found[slab * long : (slab + 1) * long]
        out[slab, 0, long : 2 * long] = found[size_x + slab * long : size_x + (slab + 1) * long]
        above, under = tiles[(slab + 1) % plan.slabs], tiles[(slab - 1) % plan.slabs]
        for pair in range(2):
            part = slice(8 * pair, 8 * pair + 8)
            here = slice(8 * slab, 8 * slab + 8)
            local = jnp.where(row % 4 < 2, above[part], under[part]) - tiles[slab][part]
            first = jumps[here, 2 * pair * size_y : (2 * pair + 1) * size_y]
            second = jumps[here, (2 * pair + 1) * size_y : (2 * pair + 2) * size_y]
            start = 2 * long + 8 * pair
            out[slab, 0, start : start + 8] = local + jnp.where(row < 4, first, second)


def return_kernel(plan, floats, wave_z, arrived, in_real, in_imag, table, *refs):
    f_high, f_low, even, odd, b_high, b_low, out_real, out_imag = refs
    long, size_y = plan.long, plan.size_y
    plane = pl.program_id(0)
    found = table_times(f_high[...], f_low[...], arrived[0, : 2 * long])
    before = (found[:long], found[long:])
    ends = jnp.concatenate((arrived[0, 2 * long : 2 * long + 8], arrived[0, 2 * long + 8 :]), axis=1)
    value = tripled(ends * end_scale(floats, ends.shape))
    sources = [dot(even[...], value), dot(odd[...], value)]
    a_real, a_imag = symbol(table, floats, wave_z, plane)
    driven = []
    for mode in range(4):
        lanes = slice((mode // 2) * size_y, (mode // 2 + 1) * size_y)
        source = sources[mode % 2][:, lanes]
        total = times(number(plan.values[mode]), (source[:long], source[long:]))
        total = plus(total, times(number(plan.weights[mode]), before))
        total = plus(total, (in_real[0, mode], in_imag[0, mode]))
        damped = damped_by(a_real, a_imag, complex(plan.values[mode]))
        driven.append(jnp.concatenate(times(damped, total), axis=0))
    back = table_times(b_high[...], b_low[...], jnp.concatenate(driven, axis=1))
    for mode in range(4):
        lanes = slice(mode * size_y, (mode + 1) * size_y)
        shape = (plan.blocks, plan.block, size_y)
        out_real[:, mode, 0] = back[:long, lanes].reshape(shape)
        out_imag[:, mode, 0] = back[long:, lanes].reshape(shape)


def leave_kernel(plan, floats, in_real, in_imag, kept, y_high, y_low, z_high, z_low, z_rest, out):
    block, rows, size_y, size_z = plan.block, plan.rows, plan.size_y, plan.size_z
    most = z_high.shape[1]

    def pair(index, carry):
        plane = 2 * index
        parts = []
        for offset in range(2):
            where = pl.ds(plane + offset, rows, stride=block)
            parts.append(jnp.concatenate((in_real[0, where, :], in_imag[0, where, :]), axis=1))
        along_y = times_table(jnp.concatenate(parts, axis=0), y_high[...], y_low[...])
        stacked = jnp.concatenate(
            (
                jnp.concatenate((along_y[:rows, :size_y], along_y[rows:, :size_y]), axis=1),
                jnp.concatenate((along_y[:rows, size_y:], along_y[rows:, size_y:]), axis=1),
            ),
            axis=0,
        )
        found = table_times(z_high[...], z_low[...], stacked[:most])
        if most < 2 * rows:
            found = found + dot(z_rest[...], tripled(stacked[most:]))
        for offset in range(2):
            add = floats[3] * kept[0, plane + offset]
            for node in range(4):
                part = found[node * size_z : (node + 1) * size_z]
                out[node, plane + offset] = part[:, offset * size_y : (offset + 1) * size_y] + add
        return carry

    lax.fori_loop(0, block // 2, pair, 0)


def whole(array):
    zeros = (0,) * array.ndim
    return pl.BlockSpec(array.shape, lambda *at: zeros)


scalars = pl.BlockSpec(memory_space=pltpu.SMEM)


def called(kernel, name, grid, in_specs, out_specs, out_shape, operands, flops=0, scratch=()):
    return pl.pallas_call(
        kernel,
        name=name,
        grid=grid,
        in_specs=in_specs,
        out_specs=out_specs,
        out_shape=out_shape,
        scratch_shapes=list(scratch),
        compiler_params=pltpu.CompilerParams(
            dimension_semantics=("arbitrary",) * len(grid), vmem_limit_bytes=56 * 1024 * 1024
        ),
    )(*operands)


def shaped(*shape):
    return jax.ShapeDtypeStruct(shape, jnp.float32)


def shards(iterate, right_side, diffusivity, velocity):
    steps = lax.axis_size("tm")
    slabs = lax.axis_size("space")
    step = lax.axis_index("tm")
    slab = lax.axis_index("space")
    nodes, long, size_z, size_y = iterate.shape[1:]
    plan = Plan(slabs, steps, long * slabs, size_z, size_y)
    size_x, padded, each = plan.size_x, plan.padded, plan.each
    rows, block, blocks, sent_rows, own = plan.rows, plan.block, plan.blocks, plan.sent, plan.own_x
    iterate, right_side = iterate[0], right_side[0]

    is_last = (step == steps - 1).astype(jnp.float32)
    floats = jnp.concatenate((velocity, is_last[None]))
    places = jnp.stack((step, slab)).astype(jnp.int32)
    wave_z = jnp.asarray(plan.z_symbols())

    forward = [(index, (index + 1) % slabs) for index in range(slabs)]
    backward = [(target, source) for source, target in forward]
    low_halo = lax.ppermute(iterate[:, -1:], "space", forward)
    high_halo = lax.ppermute(iterate[:, :1], "space", backward)

    z_tables = split_constant(plan.z_forward())
    y_tables = split_constant(plan.y_forward())
    tables = list(z_tables + y_tables)
    thick = pl.BlockSpec((4, block, size_z, size_y), lambda at: (0, at, 0, 0))
    thin = (4, 1, size_z, size_y)
    out_block = pl.BlockSpec((1, rows * block, size_y), lambda at: (at, 0, 0))
    real, imag = called(
        functools.partial(enter_kernel, plan),
        "enter",
        (blocks,),
        [
            scalars,
            thick,
            pl.BlockSpec(thin, lambda at: (0, jnp.maximum(at * block - 1, 0), 0, 0)),
            pl.BlockSpec(thin, lambda at: (0, jnp.minimum(at * block + block, long - 1), 0, 0)),
            whole(low_halo),
            whole(high_halo),
            thick,
            pl.BlockSpec((block, size_z, size_y), lambda at: (at, 0, 0)),
        ]
        + [whole(table) for table in tables],
        [out_block, out_block],
        [shaped(blocks, rows * block, size_y)] * 2,
        [floats, iterate, iterate, iterate, low_halo, high_halo, right_side, diffusivity] + tables,
        scratch=[pltpu.VMEM((4, block + 2, size_z, size_y), jnp.float32)],
    )

    by_plane = (blocks, 4, padded, block, size_y)
    plane_block = pl.BlockSpec((blocks, 4, 1, block, size_y), lambda at: (0, 0, at, 0, 0))
    mode_block = pl.BlockSpec((1, 4, long, size_y), lambda at: (at, 0, 0, 0))
    sent_block = pl.BlockSpec((1, sent_rows, size_y), lambda at: (at, 0, 0))
    local_table = plan.symbol_tables(long)
    x_forward = split_constant(plan.x_forward(long))
    x_backward = split_constant(plan.x_backward(long))
    tables = list((local_table,) + x_forward + x_backward + split_constant(plan.ends()))
    mode_real, mode_imag, sent = called(
        functools.partial(modes_kernel, plan),
        "modes",
        (padded,),
        [scalars, scalars, plane_block, plane_block] + [whole(table) for table in tables],
        [mode_block, mode_block, sent_block],
        [shaped(padded, 4, long, size_y)] * 2 + [shaped(padded, sent_rows, size_y)],
        [floats, wave_z, real.reshape(by_plane), imag.reshape(by_plane)] + tables,
    )

    arrived = lax.all_to_all(
        sent.reshape(slabs, each, sent_rows, size_y), "space", 0, 0, tiled=True
    )
    full_table = plan.symbol_tables(size_x)
    all_forward = split_constant(plan.x_forward(size_x))
    all_backward = split_constant(plan.x_backward(size_x))
    sources = tuple(tripled_constant(matrix) for matrix in plan.jump_sources())
    slab_block = pl.BlockSpec((slabs, 1, sent_rows, size_y), lambda at: (0, at, 0, 0))
    step_block = pl.BlockSpec((steps, 1, 2 * own, size_y), lambda at: (0, at, 0, 0))
    step_shape = shaped(steps, each, 2 * own, size_y)
    tables = list((full_table,) + all_forward + sources)
    last = called(
        functools.partial(last_kernel, plan),
        "last",
        (each,),
        [scalars, scalars, scalars, slab_block] + [whole(table) for table in tables],
        step_block,
        step_shape,
        [floats, wave_z, places, arrived] + tables,
    )

    gathered = lax.all_to_all(last, "tm", 0, 0, tiled=True)
    before = called(
        functools.partial(sweep_kernel, plan),
        "sweep",
        (each,),
        [scalars, scalars, scalars, step_block, whole(full_table)],
        step_block,
        step_shape,
        [floats, wave_z, places, gathered, full_table],
    )
    before = lax.all_to_all(before, "tm", 0, 0, tiled=True)

    end_block = pl.BlockSpec((slabs, 1, 16, size_y), lambda at: (0, at, 2 * long // 16, 0))
    tables = list((full_table,) + all_backward + sources + split_constant(plan.jumps()))
    back = called(
        functools.partial(driven_kernel, plan),
        "driven",
        (each,),
        [scalars, scalars, scalars, step_block, end_block] + [whole(table) for table in tables],
        slab_block,
        shaped(slabs, each, sent_rows, size_y),
        [floats, wave_z, places, before, arrived] + tables,
    )
    back = lax.all_to_all(back, "space", 0, 0, tiled=True).reshape(padded, sent_rows, size_y)

    ends = tuple(tripled_constant(matrix) for matrix in plan.end_sources())
    tables = list((local_table,) + x_forward + ends + x_backward)
    real, imag = called(
        functools.partial(return_kernel, plan),
        "return",
        (padded,),
        [scalars, scalars, sent_block, mode_block, mode_block] + [whole(table) for table in tables],
        [plane_block, plane_block],
        [shaped(*by_plane)] * 2,
        [floats, wave_z, back, mode_real, mode_imag] + tables,
    )

    z_backward = plan.z_backward()
    most = min(256, 2 * rows)
    z_tables = split_constant(z_backward[:, :most])
    rest = z_backward[:, most:] if most < 2 * rows else z_backward[:, :16]
    tables = list(split_constant(plan.y_backward()) + z_tables) + [tripled_constant(rest)]
    result = called(
        functools.partial(leave_kernel, plan),
        "leave",
        (blocks,),
        [
            scalars,
            out_block,
            out_block,
            pl.BlockSpec((1, block, size_z, size_y), lambda at: (3, at, 0, 0)),
        ]
        + [whole(table) for table in tables],
        thick,
        shaped(4, long, size_z, size_y),
        [
            floats,
            real.reshape(blocks, rows * block, size_y),
            imag.reshape(blocks, rows * block, size_y),
            iterate,
        ]
        + tables,
    )
    return result[None]


def solution(mesh):
    placed = (
        P("tm", None, "space", None, None),
        P("tm", None, "space", None, None),
        P("space", None, None),
        P(),
    )
    return jax.shard_map(
        shards,
        mesh=mesh,
        in_specs=placed,
        out_specs=P("tm", None, "space", None, None),
        check_vma=False,
    )
```

```python
import functools
import math

import jax
import jax.numpy as jnp
import numpy as np
from jax import lax
from jax.experimental import pallas as pl
from jax.experimental.pallas import tpu as pltpu
from jax.sharding import PartitionSpec as P

diffusion_number = 16.0
circulant_alpha = 0.1
MESH = pl.DeviceIdType.MESH


def collocation_matrix():
    radau_nodes = [0.08858795951270394, 0.4094668644407347, 0.7876594617608471, 1.0]
    matrix = [[0.0] * 4 for row_index in range(4)]
    for column_index in range(4):
        coefficients = [1.0]
        for other_index in range(4):
            if other_index != column_index:
                scale_value = 1.0 / (radau_nodes[column_index] - radau_nodes[other_index])
                shifted = [0.0] + [value * scale_value for value in coefficients]
                lowered = [
                    -radau_nodes[other_index] * scale_value * value for value in coefficients
                ] + [0.0]
                coefficients = [
                    left_value + right_value for left_value, right_value in zip(shifted, lowered)
                ]
        for row_index in range(4):
            total = 0.0
            for power_index in range(len(coefficients)):
                total = total + coefficients[power_index] * radau_nodes[row_index] ** (
                    power_index + 1
                ) / (power_index + 1)
            matrix[row_index][column_index] = total
    return matrix


def solve_system(matrix, target):
    count = len(target)
    rows_list = [list(matrix[row_index]) + [target[row_index]] for row_index in range(count)]
    for column in range(count):
        best_row = column
        for candidate in range(column + 1, count):
            if abs(rows_list[candidate][column]) > abs(rows_list[best_row][column]):
                best_row = candidate
        saved_row = rows_list[column]
        rows_list[column] = rows_list[best_row]
        rows_list[best_row] = saved_row
        leader = rows_list[column][column]
        for other_row in range(count):
            if other_row != column:
                factor = rows_list[other_row][column] / leader
                rows_list[other_row] = [
                    left_value - factor * right_value
                    for left_value, right_value in zip(rows_list[other_row], rows_list[column])
                ]
    return [
        rows_list[row_index][count] / rows_list[row_index][row_index] for row_index in range(count)
    ]


def node_basis():
    matrix = collocation_matrix()
    helper = [[0.0] * 4 for row_index in range(4)]
    coefficients = [0.0, 0.0, 0.0, 0.0, 1.0]
    for order in range(1, 5):
        product = [
            [
                sum((matrix[row_index][inner] * helper[inner][column] for inner in range(4)))
                for column in range(4)
            ]
            for row_index in range(4)
        ]
        for row_index in range(4):
            product[row_index][row_index] = product[row_index][row_index] + coefficients[5 - order]
        helper = product
        trace_value = sum(
            (
                sum((matrix[row_index][inner] * helper[inner][row_index] for inner in range(4)))
                for row_index in range(4)
            )
        )
        coefficients[4 - order] = -trace_value / order
    roots_list = [(0.4 + 0.9j) ** power_index for power_index in range(4)]
    for sweep in range(400):
        for root_index in range(4):
            current = roots_list[root_index]
            numer = 0.0
            for power_index in range(4, -1, -1):
                numer = numer * current + coefficients[power_index]
            denom = 1.0
            for other_index in range(4):
                if other_index != root_index:
                    denom = denom * (current - roots_list[other_index])
            roots_list[root_index] = current - numer / denom
    vectors = [[0.0] * 4 for row_index in range(4)]
    for root_index in range(4):
        shifted = [
            [
                matrix[row_index][column] - (roots_list[root_index] if row_index == column else 0.0)
                for column in range(3)
            ]
            for row_index in range(3)
        ]
        target = [-matrix[row_index][3] for row_index in range(3)]
        parts = solve_system(shifted, target) + [1.0 + 0j]
        for row_index in range(4):
            vectors[row_index][root_index] = parts[row_index]
    inverse = [[0.0] * 4 for row_index in range(4)]
    for column in range(4):
        unit = [1.0 if row_index == column else 0.0 for row_index in range(4)]
        parts = solve_system(vectors, unit)
        for row_index in range(4):
            inverse[row_index][column] = parts[row_index]
    weights = [sum((inverse[row_index][column] for column in range(4))) for row_index in range(4)]
    return (roots_list, vectors, inverse, weights)


def split_constant(matrix):
    high = matrix.astype(jnp.bfloat16)
    low = (matrix - high.astype(np.float64)).astype(jnp.bfloat16)
    return high, low


def split(value):
    high = value.astype(jnp.bfloat16)
    low = (value - high.astype(jnp.float32)).astype(jnp.bfloat16)
    return high, low


def dot(left, right):
    return jnp.dot(left, right, preferred_element_type=jnp.float32)


def table_times(high, low, value):
    value_high, value_low = split(value)
    return dot(high, value_high) + dot(high, value_low) + dot(low, value_high)


def times_table(value, high, low):
    value_high, value_low = split(value)
    return dot(value_high, high) + dot(value_low, high) + dot(value_high, low)


def tripled(value):
    high = value.astype(jnp.bfloat16).astype(jnp.float32)
    return jnp.concatenate((high, value - high, high), axis=0).astype(jnp.bfloat16)


def tripled_constant(matrix):
    high, low = split_constant(matrix)
    return np.concatenate((high, high, low), axis=1)


def complex_block(matrix):
    return np.block([[matrix.real, -matrix.imag], [matrix.imag, matrix.real]])


def fourier(rows, columns, length, sign):
    phases = np.outer(rows, columns) % length
    return np.exp(sign * 2j * np.pi * phases / length)


class Plan:
    def __init__(self, slabs, steps, size_x, size_z, size_y):
        self.slabs, self.steps = slabs, steps
        self.size_x, self.size_z, self.size_y = size_x, size_z, size_y
        self.long = long = size_x // slabs
        self.planes = size_z // 2 + 1
        each = -(-self.planes // slabs)
        while (each * slabs) % 2:
            each += 1
        self.each = each
        self.padded = each * slabs
        self.rows = 4 * self.padded
        self.block = 8
        self.blocks = long // self.block
        self.own_x = size_x // steps
        self.sent = 2 * long + 16
        self.values, self.vectors, self.inverse, self.weights = node_basis()
        self.matrix = np.array(collocation_matrix())

    def symbol_tables(self, length):
        theta_x = 2.0 * np.pi * np.arange(length)[:, None] / length
        theta_y = 2.0 * np.pi * np.arange(self.size_y)[None, :] / self.size_y
        real = diffusion_number * (2.0 * np.cos(theta_x) + 2.0 * np.cos(theta_y) - 4.0)
        ones = np.ones_like(real)
        return np.stack((real, np.sin(theta_x) * ones, np.sin(theta_y) * ones)).astype(np.float32)

    def z_symbols(self):
        theta = 2.0 * np.pi * np.arange(self.padded) / self.size_z
        return np.stack((diffusion_number * (2.0 * np.cos(theta) - 2.0), np.sin(theta))).astype(
            np.float32
        )

    def z_forward(self):
        wave = fourier(np.arange(self.padded), np.arange(self.size_z), self.size_z, -1.0)
        wave[self.planes :] = 0.0
        full = np.einsum("mn,kz->mknz", np.array(self.inverse), wave)
        full = full.reshape(self.rows, 4 * self.size_z)
        return np.concatenate((full.real, full.imag), axis=0)

    def z_backward(self):
        wave = fourier(np.arange(self.size_z), np.arange(self.padded), self.size_z, 1.0)
        weight = np.full(self.padded, 2.0)
        weight[0] = 1.0
        weight[self.planes - 1] = 1.0
        weight[self.planes :] = 0.0
        wave = wave * weight / self.size_z
        full = np.einsum("nm,zk->nzmk", np.array(self.vectors), wave)
        full = full.reshape(4 * self.size_z, self.rows)
        return np.concatenate((full.real, -full.imag), axis=1)

    def y_forward(self):
        span = np.arange(self.size_y)
        return complex_block(fourier(span, span, self.size_y, -1.0)).T

    def y_backward(self):
        span = np.arange(self.size_y)
        return complex_block(fourier(span, span, self.size_y, 1.0)).T / self.size_y

    def x_forward(self, length):
        span = np.arange(length)
        return complex_block(fourier(span, span, length, -1.0))

    def x_backward(self, length):
        span = np.arange(length)
        return complex_block(fourier(span, span, length, 1.0)) / length

    def ends(self):
        points = np.array([0, self.long - 1])
        wave = fourier(points, np.arange(self.long), self.long, 1.0) / self.long
        full = complex_block(wave)[[0, 2, 1, 3]]
        return np.concatenate((full, full, full, full), axis=0)

    def jump_sources(self):
        wave = np.arange(self.size_x)
        even = []
        for slab in range(self.slabs):
            start = slab * self.long

            def phase(point):
                return fourier(wave, np.array([point % self.size_x]), self.size_x, -1.0)[:, 0]

            first = phase(start - 1) - phase(start + self.long - 1)
            last = phase(start + self.long) - phase(start)
            even.append(np.stack((first, 1j * first, last, 1j * last), axis=1))
        return self.by_parity(even)

    def by_parity(self, blocks):
        zero = np.zeros_like(blocks[0])
        even = np.concatenate([part for block in blocks for part in (block, zero)], axis=1)
        odd = np.concatenate([part for block in blocks for part in (zero, block)], axis=1)
        return [np.concatenate((full.real, full.imag), axis=0) for full in (even, odd)]

    def end_sources(self):
        wave = np.arange(self.long)
        upper = fourier(wave, np.array([1]), self.long, 1.0)[:, 0]
        lower = np.ones_like(upper)
        return self.by_parity([np.stack((upper, 1j * upper, lower, 1j * lower), axis=1)])

    def jumps(self):
        wave = np.arange(self.size_x)
        rows = []
        for slab in range(self.slabs):
            start = slab * self.long
            points = np.array([start + self.long, start, start - 1, start + self.long - 1])
            value = fourier(points % self.size_x, wave, self.size_x, 1.0) / self.size_x
            upper, lower = value[0] - value[1], value[2] - value[3]
            full = complex_block(np.stack((upper, lower)))[[0, 2, 1, 3]]
            rows += [full, full]
        return np.concatenate(rows, axis=0)


def damped_by(real, imag, value):
    lower_real = 1.0 - (real * value.real - imag * value.imag)
    lower_imag = real * value.imag + imag * value.real
    scale = 1.0 / (lower_real * lower_real + lower_imag * lower_imag)
    return lower_real * scale, lower_imag * scale


def symbol(table, floats, wave_z, plane):
    real = table[0] + wave_z[0, plane]
    imag = -(floats[0] * table[1] + floats[1] * table[2] + floats[2] * wave_z[1, plane])
    return real, imag


def times(left, right):
    return (left[0] * right[0] - left[1] * right[1], left[0] * right[1] + left[1] * right[0])


def plus(left, right):
    return (left[0] + right[0], left[1] + right[1])


def number(value):
    value = complex(value)
    return (value.real, value.imag)


def end_scale(floats, shape):
    row = lax.broadcasted_iota(jnp.int32, shape, 0) % 4
    upper = diffusion_number - 0.5 * floats[0]
    lower = diffusion_number + 0.5 * floats[0]
    return jnp.where(row < 2, upper, lower)


def enter_kernel(plan, floats, it, below, above, low_halo, high_halo, right, diff, *refs):
    z_high, z_low, y_high, y_low, out_real, out_imag, buffer = refs
    block, rows, size_y = plan.block, plan.rows, plan.size_y
    at = pl.program_id(0)
    first, last = at == 0, at == pl.num_programs(0) - 1
    buffer[:, 1 : block + 1] = it[...]
    buffer[:, 0:1] = jnp.where(first, low_halo[...], below[...])
    buffer[:, block + 1 :] = jnp.where(last, high_halo[...], above[...])
    nodes = plan.matrix.sum(axis=1)
    size_z = plan.size_z

    def driving(plane):
        factor = diffusion_number * (diff[plane] - 1.0)
        terms = []
        for node in range(4):
            center = buffer[node, plane + 1]
            upper, lower = buffer[node, plane + 2], buffer[node, plane]
            z_up, z_down = pltpu.roll(center, size_z - 1, 0), pltpu.roll(center, 1, 0)
            y_up, y_down = pltpu.roll(center, size_y - 1, 1), pltpu.roll(center, 1, 1)
            laplace = (upper + lower) + (z_up + z_down) + (y_up + y_down) - 6.0 * center
            terms.append(factor * laplace)
        transport = (
            floats[0] * (upper - lower) + floats[1] * (y_up - y_down) + floats[2] * (z_up - z_down)
        )
        operated = floats[3] * (diffusion_number * laplace - 0.5 * transport)
        kept = floats[3] * center
        result = []
        for row in range(4):
            total = right[row, plane] + (float(nodes[row]) * operated - kept)
            for column in range(4):
                total = total + float(plan.matrix[row, column]) * terms[column]
            result.append(total)
        return jnp.concatenate(result, axis=0)

    def pair(index, carry):
        plane = 2 * index
        both = jnp.concatenate((driving(plane), driving(plane + 1)), axis=1)
        along_z = table_times(z_high[...], z_low[...], both)
        real, imag = along_z[:rows], along_z[rows:]
        stacked = jnp.concatenate(
            (
                jnp.concatenate((real[:, :size_y], imag[:, :size_y]), axis=1),
                jnp.concatenate((real[:, size_y:], imag[:, size_y:]), axis=1),
            ),
            axis=0,
        )
        along_y = times_table(stacked, y_high[...], y_low[...])
        for offset in range(2):
            part = along_y[offset * rows : (offset + 1) * rows]
            where = pl.ds(plane + offset, rows, stride=block)
            out_real[0, where, :] = part[:, :size_y]
            out_imag[0, where, :] = part[:, size_y:]
        return carry

    lax.fori_loop(0, block // 2, pair, 0)


def modes_kernel(plan, floats, wave_z, in_real, in_imag, table, *refs):
    f_high, f_low, b_high, b_low, e_high, e_low, out_real, out_imag, sent = refs
    long, size_y = plan.long, plan.size_y
    plane = pl.program_id(0)
    real = [in_real[:, mode, 0].reshape(long, size_y) for mode in range(4)]
    imag = [in_imag[:, mode, 0].reshape(long, size_y) for mode in range(4)]
    value = jnp.concatenate(
        (jnp.concatenate(real, axis=1), jnp.concatenate(imag, axis=1)), axis=0
    )
    spectrum = table_times(f_high[...], f_low[...], value)
    a_real, a_imag = symbol(table, floats, wave_z, plane)
    total, inner = None, []
    for mode in range(4):
        lanes = slice(mode * size_y, (mode + 1) * size_y)
        part = (spectrum[:long, lanes], spectrum[long:, lanes])
        out_real[0, mode], out_imag[0, mode] = part
        part = times(damped_by(a_real, a_imag, complex(plan.values[mode])), part)
        total = part if total is None else plus(total, part)
        inner.append(jnp.concatenate(part, axis=0))
    last = table_times(b_high[...], b_low[...], jnp.concatenate(total, axis=0))
    sent[0, : 2 * long] = last
    ends = table_times(e_high[...], e_low[...], jnp.concatenate(inner, axis=1))[:8]
    upper = lax.broadcasted_iota(jnp.int32, (8, size_y), 0) < 4
    for pair in range(2):
        even = ends[:, 2 * pair * size_y : (2 * pair + 1) * size_y]
        odd = ends[:, (2 * pair + 1) * size_y : (2 * pair + 2) * size_y]
        start = 2 * long + 8 * pair
        sent[0, start : start + 8] = jnp.where(upper, even, odd)


def end_spectra(plan, floats, tiles, even, odd):
    size_x, size_y = plan.size_x, plan.size_y
    pairs = []
    for pair in range(2):
        rows = jnp.concatenate([tiles[slab][8 * pair : 8 * pair + 8] for slab in range(plan.slabs)])
        pairs.append(rows * end_scale(floats, rows.shape))
    value = tripled(jnp.concatenate(pairs, axis=1))
    found = [dot(even[...], value), dot(odd[...], value)]
    result = []
    for mode in range(4):
        lanes = slice((mode // 2) * size_y, (mode // 2 + 1) * size_y)
        part = found[mode % 2][:, lanes]
        result.append(times(number(plan.values[mode]), (part[:size_x], part[size_x:])))
    return result


def spread(plan, floats, wave_z, *refs):
    (sent, table, f_high, f_low, even, odd, b_high, b_low, j_high, j_low, out) = refs[:11]
    (x_in, f_send, f_all, growth, c_send, c_all, s_send, s_all, d_send, d_all, x_out) = refs[11:22]
    (x_sems, f_sems, c_sems, s_sems, d_sems, y_sems, own_in, own_out) = refs[22:]
    slabs, steps, each = plan.slabs, plan.steps, plan.each
    long, size_x, size_y, own = plan.long, plan.size_x, plan.size_y, plan.own_x
    half, pairs = size_x // 2, steps // 2
    step, slab = lax.axis_index("tm"), lax.axis_index("space")
    parity, place = step % 2, step // 2
    other = (step + 1 - 2 * parity, slab)

    def peer(index):
        return (2 * index + parity, slab)

    def slab_peer(index):
        return (step, index)

    barrier = pltpu.get_barrier_semaphore()
    neighbours = [other]
    neighbours += [slab_peer((slab + shift) % slabs) for shift in range(1, slabs)]
    neighbours += [peer((place + shift) % pairs) for shift in range(1, pairs)]
    for device in neighbours:
        pl.semaphore_signal(barrier, inc=1, device_id=device, device_id_type=MESH)
    pl.semaphore_wait(barrier, len(neighbours))

    def remote(source, target, sems, plane, device):
        return pltpu.make_async_remote_copy(
            src_ref=source,
            dst_ref=target,
            send_sem=sems.at[0, plane],
            recv_sem=sems.at[1, plane],
            device_id=device,
            device_id_type=MESH,
        )

    def await_all(ref, sems, kind, plane):
        pltpu.make_async_copy(ref, ref, sems.at[kind, plane]).wait()

    mine = pltpu.make_async_copy(sent.at[pl.ds(slab * each, each)], x_in.at[slab], own_in)
    mine.start()

    def start_plane(plane, carry):
        for shift in range(1, slabs):
            target = (slab + shift) % slabs
            remote(
                sent.at[target * each + plane],
                x_in.at[slab, plane],
                x_sems,
                plane,
                slab_peer(target),
            ).start()
        return carry

    lax.fori_loop(0, each, start_plane, 0)
    mine.wait()

    def symbols(plane, start, count):
        rows = pl.ds(start, count)
        tables = [table[index, rows] for index in range(3)]
        return symbol(tables, floats, wave_z, slab * each + plane)

    def grown(plane, start, count):
        a_real, a_imag = symbols(plane, start, count)
        total = None
        for mode in range(4):
            damped = damped_by(a_real, a_imag, complex(plan.values[mode]))
            term = times(number(plan.weights[mode]), damped)
            total = term if total is None else plus(total, term)
        return total

    def spectrum_stage(plane):
        if slabs > 1:
            await_all(x_in.at[pl.ds(0, slabs - 1), plane], x_sems, 1, plane)
        arrived = [x_in[index, plane] for index in range(slabs)]
        value = jnp.concatenate(
            [part[:long] for part in arrived] + [part[long : 2 * long] for part in arrived], axis=0
        )
        found = table_times(f_high[...], f_low[...], value)
        total = (found[:size_x], found[size_x:])
        sources = end_spectra(plan, floats, [part[2 * long :] for part in arrived], even, odd)
        a_real, a_imag = symbols(plane, 0, size_x)
        for mode in range(4):
            damped = damped_by(a_real, a_imag, complex(plan.values[mode]))
            total = plus(total, times(damped, sources[mode]))
        for index in range(2):
            rows = slice(index * half, (index + 1) * half)
            lower, upper = total[index][:half], total[index][half:]
            f_send[plane, rows] = jnp.where(parity == 0, upper, lower)
            f_all[plane, parity, rows] = jnp.where(parity == 0, lower, upper)
        remote(f_send.at[plane], f_all.at[plane, parity], f_sems, plane, other).start()

    def pair_stage(plane):
        factor = grown(plane, pl.multiple_of(parity * half, half), half)
        growth[plane, :half], growth[plane, half:] = factor
        await_all(f_send.at[plane], f_sems, 1, plane)
        early = (f_all[plane, 0, :half], f_all[plane, 0, half:])
        later = (f_all[plane, 1, :half], f_all[plane, 1, half:])
        total = plus(later, times(factor, early))
        for index in range(pairs):
            rows = slice(index * own, (index + 1) * own)
            c_send[index, plane, :own] = total[0][rows]
            c_send[index, plane, own:] = total[1][rows]
        c_all[place, plane] = c_send[place, plane]
        for shift in range(1, pairs):
            target = (place + shift) % pairs
            remote(
                c_send.at[target, plane], c_all.at[place, plane], c_sems, plane, peer(target)
            ).start()

    def sweep_stage(plane):
        factor = grown(plane, pl.multiple_of(parity * half + place * own, own), own)
        factor = times(factor, factor)
        if pairs > 1:
            await_all(c_all.at[pl.ds(0, pairs - 1), plane], c_sems, 1, plane)
        fields = [(c_all[index, plane, :own], c_all[index, plane, own:]) for index in range(pairs)]
        total, power = fields[0], factor
        for index in range(1, pairs):
            total = plus(fields[index], times(factor, total))
            power = times(factor, power)
        lower = (1.0 - circulant_alpha * power[0], -circulant_alpha * power[1])
        scale = circulant_alpha / (lower[0] * lower[0] + lower[1] * lower[1])
        current = times(total, (lower[0] * scale, -lower[1] * scale))
        for index in range(pairs):
            s_send[index, plane, :own] = current[0]
            s_send[index, plane, own:] = current[1]
            current = plus(fields[index], times(factor, current))
        s_all[place, plane] = s_send[place, plane]
        for shift in range(1, pairs):
            target = (place + shift) % pairs
            remote(
                s_send.at[target, plane], s_all.at[place, plane], s_sems, plane, peer(target)
            ).start()

    def start_stage(plane):
        if pairs > 1:
            await_all(s_all.at[pl.ds(0, pairs - 1), plane], s_sems, 1, plane)
        early = tuple(
            jnp.concatenate([s_all[index, plane, rows] for index in range(pairs)], axis=0)
            for rows in (slice(0, own), slice(own, 2 * own))
        )
        field = (f_all[plane, 0, :half], f_all[plane, 0, half:])
        later = plus(field, times((growth[plane, :half], growth[plane, half:]), early))
        for index in range(2):
            rows = slice(index * half, (index + 1) * half)
            d_send[plane, rows] = jnp.where(parity == 0, later[index], early[index])
            d_all[plane, parity, rows] = jnp.where(parity == 0, early[index], later[index])
        remote(d_send.at[plane], d_all.at[plane, parity], d_sems, plane, other).start()

    def return_stage(plane):
        await_all(d_send.at[plane], d_sems, 1, plane)
        real = jnp.concatenate((d_all[plane, 0, :half], d_all[plane, 1, :half]), axis=0)
        imag = jnp.concatenate((d_all[plane, 0, half:], d_all[plane, 1, half:]), axis=0)
        found = table_times(b_high[...], b_low[...], jnp.concatenate((real, imag), axis=0))
        tiles = [x_in[index, plane, 2 * long :] for index in range(slabs)]
        sources = end_spectra(plan, floats, tiles, even, odd)
        a_real, a_imag = symbols(plane, 0, size_x)
        driven = []
        for mode in range(4):
            damped = damped_by(a_real, a_imag, complex(plan.values[mode]))
            weighted = times(number(plan.weights[mode]), (real, imag))
            driven.append(jnp.concatenate(times(damped, plus(weighted, sources[mode])), axis=0))
        jumps = table_times(j_high[...], j_low[...], jnp.concatenate(driven, axis=1))
        row = lax.broadcasted_iota(jnp.int32, (8, size_y), 0)
        for index in range(slabs):
            first = index * long
            x_out[index, plane, :long] = found[first : first + long]
            x_out[index, plane, long : 2 * long] = found[size_x + first : size_x + first + long]
            above, under = tiles[(index + 1) % slabs], tiles[(index - 1) % slabs]
            for pair in range(2):
                part = slice(8 * pair, 8 * pair + 8)
                here = slice(8 * index, 8 * index + 8)
                local = jnp.where(row % 4 < 2, above[part], under[part]) - tiles[index][part]
                lower = jumps[here, 2 * pair * size_y : (2 * pair + 1) * size_y]
                upper = jumps[here, (2 * pair + 1) * size_y : (2 * pair + 2) * size_y]
                start = 2 * long + 8 * pair
                x_out[index, plane, start : start + 8] = local + jnp.where(row < 4, lower, upper)
        pltpu.make_async_copy(
            x_out.at[slab, plane], out.at[slab, plane], own_out.at[plane]
        ).start()
        for shift in range(1, slabs):
            target = (slab + shift) % slabs
            remote(
                x_out.at[target, plane], out.at[slab, plane], y_sems, plane, slab_peer(target)
            ).start()

    stages = (spectrum_stage, pair_stage, sweep_stage, start_stage, return_stage)

    def iteration(time, carry):
        for delay in reversed(range(len(stages))):
            plane = time - delay

            @pl.when(jnp.logical_and(plane >= 0, plane < each))
            def _():
                stages[delay](plane)

        return carry

    lax.fori_loop(0, each + len(stages) - 1, iteration, 0)

    def finish(plane, carry):
        await_all(f_send.at[plane], f_sems, 0, plane)
        await_all(d_send.at[plane], d_sems, 0, plane)
        if pairs > 1:
            await_all(c_send.at[pl.ds(0, pairs - 1), plane], c_sems, 0, plane)
            await_all(s_send.at[pl.ds(0, pairs - 1), plane], s_sems, 0, plane)
        if slabs > 1:
            await_all(x_in.at[pl.ds(0, slabs - 1), plane], x_sems, 0, plane)
            await_all(x_out.at[pl.ds(0, slabs - 1), plane], y_sems, 0, plane)
            await_all(x_out.at[pl.ds(0, slabs - 1), plane], y_sems, 1, plane)
        pltpu.make_async_copy(
            x_out.at[slab, plane], out.at[slab, plane], own_out.at[plane]
        ).wait()
        return carry

    lax.fori_loop(0, each, finish, 0)


def return_kernel(plan, floats, wave_z, arrived, in_real, in_imag, table, *refs):
    f_high, f_low, even, odd, b_high, b_low, out_real, out_imag = refs
    long, size_y = plan.long, plan.size_y
    plane = pl.program_id(0)
    found = table_times(f_high[...], f_low[...], arrived[0, : 2 * long])
    before = (found[:long], found[long:])
    ends = jnp.concatenate((arrived[0, 2 * long : 2 * long + 8], arrived[0, 2 * long + 8 :]), axis=1)
    value = tripled(ends * end_scale(floats, ends.shape))
    sources = [dot(even[...], value), dot(odd[...], value)]
    a_real, a_imag = symbol(table, floats, wave_z, plane)
    driven = []
    for mode in range(4):
        lanes = slice((mode // 2) * size_y, (mode // 2 + 1) * size_y)
        source = sources[mode % 2][:, lanes]
        total = times(number(plan.values[mode]), (source[:long], source[long:]))
        total = plus(total, times(number(plan.weights[mode]), before))
        total = plus(total, (in_real[0, mode], in_imag[0, mode]))
        damped = damped_by(a_real, a_imag, complex(plan.values[mode]))
        driven.append(jnp.concatenate(times(damped, total), axis=0))
    back = table_times(b_high[...], b_low[...], jnp.concatenate(driven, axis=1))
    for mode in range(4):
        lanes = slice(mode * size_y, (mode + 1) * size_y)
        shape = (plan.blocks, plan.block, size_y)
        out_real[:, mode, 0] = back[:long, lanes].reshape(shape)
        out_imag[:, mode, 0] = back[long:, lanes].reshape(shape)


def leave_kernel(plan, floats, in_real, in_imag, kept, y_high, y_low, z_high, z_low, z_rest, out):
    block, rows, size_y, size_z = plan.block, plan.rows, plan.size_y, plan.size_z
    most = z_high.shape[1]

    def pair(index, carry):
        plane = 2 * index
        parts = []
        for offset in range(2):
            where = pl.ds(plane + offset, rows, stride=block)
            parts.append(jnp.concatenate((in_real[0, where, :], in_imag[0, where, :]), axis=1))
        along_y = times_table(jnp.concatenate(parts, axis=0), y_high[...], y_low[...])
        stacked = jnp.concatenate(
            (
                jnp.concatenate((along_y[:rows, :size_y], along_y[rows:, :size_y]), axis=1),
                jnp.concatenate((along_y[:rows, size_y:], along_y[rows:, size_y:]), axis=1),
            ),
            axis=0,
        )
        found = table_times(z_high[...], z_low[...], stacked[:most])
        if most < 2 * rows:
            found = found + dot(z_rest[...], tripled(stacked[most:]))
        for offset in range(2):
            add = floats[3] * kept[0, plane + offset]
            for node in range(4):
                part = found[node * size_z : (node + 1) * size_z]
                out[node, plane + offset] = part[:, offset * size_y : (offset + 1) * size_y] + add
        return carry

    lax.fori_loop(0, block // 2, pair, 0)


def whole(array):
    zeros = (0,) * array.ndim
    return pl.BlockSpec(array.shape, lambda *at: zeros)


scalars = pl.BlockSpec(memory_space=pltpu.SMEM)


def called(kernel, name, grid, in_specs, out_specs, out_shape, operands, flops=0, scratch=()):
    return pl.pallas_call(
        kernel,
        name=name,
        grid=grid,
        in_specs=in_specs,
        out_specs=out_specs,
        out_shape=out_shape,
        scratch_shapes=list(scratch),
        compiler_params=pltpu.CompilerParams(
            dimension_semantics=("arbitrary",) * len(grid), vmem_limit_bytes=56 * 1024 * 1024
        ),
    )(*operands)


def shaped(*shape):
    return jax.ShapeDtypeStruct(shape, jnp.float32)


def shards(iterate, right_side, diffusivity, velocity):
    steps = lax.axis_size("tm")
    slabs = lax.axis_size("space")
    step = lax.axis_index("tm")
    nodes, long, size_z, size_y = iterate.shape[1:]
    plan = Plan(slabs, steps, long * slabs, size_z, size_y)
    size_x, padded, each = plan.size_x, plan.padded, plan.each
    rows, block, blocks, sent_rows, own = plan.rows, plan.block, plan.blocks, plan.sent, plan.own_x
    iterate, right_side = iterate[0], right_side[0]

    is_last = (step == steps - 1).astype(jnp.float32)
    floats = jnp.concatenate((velocity, is_last[None]))
    wave_z = jnp.asarray(plan.z_symbols())

    forward = [(index, (index + 1) % slabs) for index in range(slabs)]
    backward = [(target, source) for source, target in forward]
    low_halo = lax.ppermute(iterate[:, -1:], "space", forward)
    high_halo = lax.ppermute(iterate[:, :1], "space", backward)

    z_tables = split_constant(plan.z_forward())
    y_tables = split_constant(plan.y_forward())
    tables = list(z_tables + y_tables)
    thick = pl.BlockSpec((4, block, size_z, size_y), lambda at: (0, at, 0, 0))
    thin = (4, 1, size_z, size_y)
    out_block = pl.BlockSpec((1, rows * block, size_y), lambda at: (at, 0, 0))
    real, imag = called(
        functools.partial(enter_kernel, plan),
        "enter",
        (blocks,),
        [
            scalars,
            thick,
            pl.BlockSpec(thin, lambda at: (0, jnp.maximum(at * block - 1, 0), 0, 0)),
            pl.BlockSpec(thin, lambda at: (0, jnp.minimum(at * block + block, long - 1), 0, 0)),
            whole(low_halo),
            whole(high_halo),
            thick,
            pl.BlockSpec((block, size_z, size_y), lambda at: (at, 0, 0)),
        ]
        + [whole(table) for table in tables],
        [out_block, out_block],
        [shaped(blocks, rows * block, size_y)] * 2,
        [floats, iterate, iterate, iterate, low_halo, high_halo, right_side, diffusivity] + tables,
        scratch=[pltpu.VMEM((4, block + 2, size_z, size_y), jnp.float32)],
    )

    by_plane = (blocks, 4, padded, block, size_y)
    plane_block = pl.BlockSpec((blocks, 4, 1, block, size_y), lambda at: (0, 0, at, 0, 0))
    mode_block = pl.BlockSpec((1, 4, long, size_y), lambda at: (at, 0, 0, 0))
    sent_block = pl.BlockSpec((1, sent_rows, size_y), lambda at: (at, 0, 0))
    local_table = plan.symbol_tables(long)
    x_forward = split_constant(plan.x_forward(long))
    x_backward = split_constant(plan.x_backward(long))
    tables = list((local_table,) + x_forward + x_backward + split_constant(plan.ends()))
    mode_real, mode_imag, sent = called(
        functools.partial(modes_kernel, plan),
        "modes",
        (padded,),
        [scalars, scalars, plane_block, plane_block] + [whole(table) for table in tables],
        [mode_block, mode_block, sent_block],
        [shaped(padded, 4, long, size_y)] * 2 + [shaped(padded, sent_rows, size_y)],
        [floats, wave_z, real.reshape(by_plane), imag.reshape(by_plane)] + tables,
    )

    tables = [plan.symbol_tables(size_x)] + list(split_constant(plan.x_forward(size_x)))
    tables += [tripled_constant(matrix) for matrix in plan.jump_sources()]
    tables += list(split_constant(plan.x_backward(size_x)) + split_constant(plan.jumps()))
    half, pairs = size_x // 2, steps // 2
    anywhere = pl.BlockSpec(memory_space=pl.ANY)

    def held(*shape):
        return pltpu.VMEM(shape, jnp.float32)

    halves, parts = (each, 2 * half, size_y), (pairs, each, 2 * own, size_y)
    both = (each, 2, 2 * half, size_y)
    slots = (slabs, each, sent_rows, size_y)
    back = pl.pallas_call(
        functools.partial(spread, plan),
        name="spread",
        in_specs=[scalars, scalars, anywhere]
        + [pl.BlockSpec(memory_space=pltpu.VMEM) for table in tables],
        out_specs=anywhere,
        out_shape=shaped(*slots),
        scratch_shapes=[
            held(*slots),
            held(*halves),
            held(*both),
            held(*halves),
            held(*parts),
            held(*parts),
            held(*parts),
            held(*parts),
            held(*halves),
            held(*both),
            held(*slots),
        ]
        + [pltpu.SemaphoreType.DMA((2, each))] * 6
        + [pltpu.SemaphoreType.DMA, pltpu.SemaphoreType.DMA((each,))],
        compiler_params=pltpu.CompilerParams(
            collective_id=0, has_side_effects=True, vmem_limit_bytes=56 * 1024 * 1024
        ),
    )(floats, wave_z, sent, *tables).reshape(padded, sent_rows, size_y)

    ends = tuple(tripled_constant(matrix) for matrix in plan.end_sources())
    tables = list((local_table,) + x_forward + ends + x_backward)
    real, imag = called(
        functools.partial(return_kernel, plan),
        "return",
        (padded,),
        [scalars, scalars, sent_block, mode_block, mode_block] + [whole(table) for table in tables],
        [plane_block, plane_block],
        [shaped(*by_plane)] * 2,
        [floats, wave_z, back, mode_real, mode_imag] + tables,
    )

    z_backward = plan.z_backward()
    most = min(256, 2 * rows)
    z_tables = split_constant(z_backward[:, :most])
    rest = z_backward[:, most:] if most < 2 * rows else z_backward[:, :16]
    tables = list(split_constant(plan.y_backward()) + z_tables) + [tripled_constant(rest)]
    result = called(
        functools.partial(leave_kernel, plan),
        "leave",
        (blocks,),
        [
            scalars,
            out_block,
            out_block,
            pl.BlockSpec((1, block, size_z, size_y), lambda at: (3, at, 0, 0)),
        ]
        + [whole(table) for table in tables],
        thick,
        shaped(4, long, size_z, size_y),
        [
            floats,
            real.reshape(blocks, rows * block, size_y),
            imag.reshape(blocks, rows * block, size_y),
            iterate,
        ]
        + tables,
    )
    return result[None]


def solution(mesh):
    placed = (
        P("tm", None, "space", None, None),
        P("tm", None, "space", None, None),
        P("space", None, None),
        P(),
    )
    return jax.shard_map(
        shards,
        mesh=mesh,
        in_specs=placed,
        out_specs=P("tm", None, "space", None, None),
        check_vma=False,
    )
```

```python
import functools
import math

import jax
import jax.numpy as jnp
import numpy as np
from jax import lax
from jax.experimental import pallas as pl
from jax.experimental.pallas import tpu as pltpu
from jax.sharding import PartitionSpec as P

diffusion_number = 16.0
circulant_alpha = 0.1
MESH = pl.DeviceIdType.MESH


def collocation_matrix():
    radau_nodes = [0.08858795951270394, 0.4094668644407347, 0.7876594617608471, 1.0]
    matrix = [[0.0] * 4 for row_index in range(4)]
    for column_index in range(4):
        coefficients = [1.0]
        for other_index in range(4):
            if other_index != column_index:
                scale_value = 1.0 / (radau_nodes[column_index] - radau_nodes[other_index])
                shifted = [0.0] + [value * scale_value for value in coefficients]
                lowered = [
                    -radau_nodes[other_index] * scale_value * value for value in coefficients
                ] + [0.0]
                coefficients = [
                    left_value + right_value for left_value, right_value in zip(shifted, lowered)
                ]
        for row_index in range(4):
            total = 0.0
            for power_index in range(len(coefficients)):
                total = total + coefficients[power_index] * radau_nodes[row_index] ** (
                    power_index + 1
                ) / (power_index + 1)
            matrix[row_index][column_index] = total
    return matrix


def solve_system(matrix, target):
    count = len(target)
    rows_list = [list(matrix[row_index]) + [target[row_index]] for row_index in range(count)]
    for column in range(count):
        best_row = column
        for candidate in range(column + 1, count):
            if abs(rows_list[candidate][column]) > abs(rows_list[best_row][column]):
                best_row = candidate
        saved_row = rows_list[column]
        rows_list[column] = rows_list[best_row]
        rows_list[best_row] = saved_row
        leader = rows_list[column][column]
        for other_row in range(count):
            if other_row != column:
                factor = rows_list[other_row][column] / leader
                rows_list[other_row] = [
                    left_value - factor * right_value
                    for left_value, right_value in zip(rows_list[other_row], rows_list[column])
                ]
    return [
        rows_list[row_index][count] / rows_list[row_index][row_index] for row_index in range(count)
    ]


def node_basis():
    matrix = collocation_matrix()
    helper = [[0.0] * 4 for row_index in range(4)]
    coefficients = [0.0, 0.0, 0.0, 0.0, 1.0]
    for order in range(1, 5):
        product = [
            [
                sum((matrix[row_index][inner] * helper[inner][column] for inner in range(4)))
                for column in range(4)
            ]
            for row_index in range(4)
        ]
        for row_index in range(4):
            product[row_index][row_index] = product[row_index][row_index] + coefficients[5 - order]
        helper = product
        trace_value = sum(
            (
                sum((matrix[row_index][inner] * helper[inner][row_index] for inner in range(4)))
                for row_index in range(4)
            )
        )
        coefficients[4 - order] = -trace_value / order
    roots_list = [(0.4 + 0.9j) ** power_index for power_index in range(4)]
    for sweep in range(400):
        for root_index in range(4):
            current = roots_list[root_index]
            numer = 0.0
            for power_index in range(4, -1, -1):
                numer = numer * current + coefficients[power_index]
            denom = 1.0
            for other_index in range(4):
                if other_index != root_index:
                    denom = denom * (current - roots_list[other_index])
            roots_list[root_index] = current - numer / denom
    vectors = [[0.0] * 4 for row_index in range(4)]
    for root_index in range(4):
        shifted = [
            [
                matrix[row_index][column] - (roots_list[root_index] if row_index == column else 0.0)
                for column in range(3)
            ]
            for row_index in range(3)
        ]
        target = [-matrix[row_index][3] for row_index in range(3)]
        parts = solve_system(shifted, target) + [1.0 + 0j]
        for row_index in range(4):
            vectors[row_index][root_index] = parts[row_index]
    inverse = [[0.0] * 4 for row_index in range(4)]
    for column in range(4):
        unit = [1.0 if row_index == column else 0.0 for row_index in range(4)]
        parts = solve_system(vectors, unit)
        for row_index in range(4):
            inverse[row_index][column] = parts[row_index]
    weights = [sum((inverse[row_index][column] for column in range(4))) for row_index in range(4)]
    return (roots_list, vectors, inverse, weights)


def split_constant(matrix):
    high = matrix.astype(jnp.bfloat16)
    low = (matrix - high.astype(np.float64)).astype(jnp.bfloat16)
    return high, low


def split(value):
    high = value.astype(jnp.bfloat16)
    low = (value - high.astype(jnp.float32)).astype(jnp.bfloat16)
    return high, low


def dot(left, right):
    return jnp.dot(left, right, preferred_element_type=jnp.float32)


def table_times(high, low, value):
    value_high, value_low = split(value)
    return dot(high, value_high) + dot(high, value_low) + dot(low, value_high)


def times_table(value, high, low):
    value_high, value_low = split(value)
    return dot(value_high, high) + dot(value_low, high) + dot(value_high, low)


def tripled(value):
    high = value.astype(jnp.bfloat16).astype(jnp.float32)
    return jnp.concatenate((high, value - high, high), axis=0).astype(jnp.bfloat16)


def tripled_constant(matrix):
    high, low = split_constant(matrix)
    return np.concatenate((high, high, low), axis=1)


def complex_block(matrix):
    return np.block([[matrix.real, -matrix.imag], [matrix.imag, matrix.real]])


def fourier(rows, columns, length, sign):
    phases = np.outer(rows, columns) % length
    return np.exp(sign * 2j * np.pi * phases / length)


class Plan:
    def __init__(self, slabs, steps, size_x, size_z, size_y):
        self.slabs, self.steps = slabs, steps
        self.size_x, self.size_z, self.size_y = size_x, size_z, size_y
        self.long = long = size_x // slabs
        self.planes = size_z // 2 + 1
        each = -(-self.planes // slabs)
        while (each * slabs) % 2:
            each += 1
        self.each = each
        self.padded = each * slabs
        self.rows = 4 * self.padded
        self.block = 8
        self.blocks = long // self.block
        self.own_x = size_x // steps
        self.sent = 2 * long + 16
        self.values, self.vectors, self.inverse, self.weights = node_basis()
        self.matrix = np.array(collocation_matrix())

    def symbol_tables(self, length):
        theta_x = 2.0 * np.pi * np.arange(length)[:, None] / length
        theta_y = 2.0 * np.pi * np.arange(self.size_y)[None, :] / self.size_y
        real = diffusion_number * (2.0 * np.cos(theta_x) + 2.0 * np.cos(theta_y) - 4.0)
        ones = np.ones_like(real)
        return np.stack((real, np.sin(theta_x) * ones, np.sin(theta_y) * ones)).astype(np.float32)

    def z_symbols(self):
        theta = 2.0 * np.pi * np.arange(self.padded) / self.size_z
        return np.stack((diffusion_number * (2.0 * np.cos(theta) - 2.0), np.sin(theta))).astype(
            np.float32
        )

    def z_forward(self):
        wave = fourier(np.arange(self.padded), np.arange(self.size_z), self.size_z, -1.0)
        wave[self.planes :] = 0.0
        full = np.einsum("mn,kz->mknz", np.array(self.inverse), wave)
        full = full.reshape(self.rows, 4 * self.size_z)
        return np.concatenate((full.real, full.imag), axis=0)

    def z_backward(self):
        wave = fourier(np.arange(self.size_z), np.arange(self.padded), self.size_z, 1.0)
        weight = np.full(self.padded, 2.0)
        weight[0] = 1.0
        weight[self.planes - 1] = 1.0
        weight[self.planes :] = 0.0
        wave = wave * weight / self.size_z
        full = np.einsum("nm,zk->nzmk", np.array(self.vectors), wave)
        full = full.reshape(4 * self.size_z, self.rows)
        return np.concatenate((full.real, -full.imag), axis=1)

    def y_forward(self):
        span = np.arange(self.size_y)
        return complex_block(fourier(span, span, self.size_y, -1.0)).T

    def y_backward(self):
        span = np.arange(self.size_y)
        return complex_block(fourier(span, span, self.size_y, 1.0)).T / self.size_y

    def x_forward(self, length):
        span = np.arange(length)
        return complex_block(fourier(span, span, length, -1.0))

    def x_backward(self, length):
        span = np.arange(length)
        return complex_block(fourier(span, span, length, 1.0)) / length

    def ends(self):
        points = np.array([0, self.long - 1])
        wave = fourier(points, np.arange(self.long), self.long, 1.0) / self.long
        full = complex_block(wave)[[0, 2, 1, 3]]
        return np.concatenate((full, full, full, full), axis=0)

    def jump_sources(self):
        wave = np.arange(self.size_x)
        even = []
        for slab in range(self.slabs):
            start = slab * self.long

            def phase(point):
                return fourier(wave, np.array([point % self.size_x]), self.size_x, -1.0)[:, 0]

            first = phase(start - 1) - phase(start + self.long - 1)
            last = phase(start + self.long) - phase(start)
            even.append(np.stack((first, 1j * first, last, 1j * last), axis=1))
        return self.by_parity(even)

    def by_parity(self, blocks):
        zero = np.zeros_like(blocks[0])
        even = np.concatenate([part for block in blocks for part in (block, zero)], axis=1)
        odd = np.concatenate([part for block in blocks for part in (zero, block)], axis=1)
        return [np.concatenate((full.real, full.imag), axis=0) for full in (even, odd)]

    def end_sources(self):
        wave = np.arange(self.long)
        upper = fourier(wave, np.array([1]), self.long, 1.0)[:, 0]
        lower = np.ones_like(upper)
        return self.by_parity([np.stack((upper, 1j * upper, lower, 1j * lower), axis=1)])

    def jumps(self):
        wave = np.arange(self.size_x)
        rows = []
        for slab in range(self.slabs):
            start = slab * self.long
            points = np.array([start + self.long, start, start - 1, start + self.long - 1])
            value = fourier(points % self.size_x, wave, self.size_x, 1.0) / self.size_x
            upper, lower = value[0] - value[1], value[2] - value[3]
            full = complex_block(np.stack((upper, lower)))[[0, 2, 1, 3]]
            rows += [full, full]
        return np.concatenate(rows, axis=0)


def damped_by(real, imag, value):
    lower_real = 1.0 - (real * value.real - imag * value.imag)
    lower_imag = real * value.imag + imag * value.real
    scale = 1.0 / (lower_real * lower_real + lower_imag * lower_imag)
    return lower_real * scale, lower_imag * scale


def symbol(table, floats, wave_z, plane):
    real = table[0] + wave_z[0, plane]
    imag = -(floats[0] * table[1] + floats[1] * table[2] + floats[2] * wave_z[1, plane])
    return real, imag


def times(left, right):
    return (left[0] * right[0] - left[1] * right[1], left[0] * right[1] + left[1] * right[0])


def plus(left, right):
    return (left[0] + right[0], left[1] + right[1])


def number(value):
    value = complex(value)
    return (value.real, value.imag)


def end_scale(floats, shape):
    row = lax.broadcasted_iota(jnp.int32, shape, 0) % 4
    upper = diffusion_number - 0.5 * floats[0]
    lower = diffusion_number + 0.5 * floats[0]
    return jnp.where(row < 2, upper, lower)


def enter_kernel(plan, floats, it, below, above, low_halo, high_halo, right, diff, *refs):
    z_high, z_low, y_high, y_low, out, buffer = refs
    block, rows, size_y = plan.block, plan.rows, plan.size_y
    at = pl.program_id(0)
    first, last = at == 0, at == pl.num_programs(0) - 1
    buffer[:, 1 : block + 1] = it[...]
    buffer[:, 0:1] = jnp.where(first, low_halo[...], below[...])
    buffer[:, block + 1 :] = jnp.where(last, high_halo[...], above[...])
    nodes = plan.matrix.sum(axis=1)
    size_z = plan.size_z

    def driving(plane):
        factor = diffusion_number * (diff[plane] - 1.0)
        terms = []
        for node in range(4):
            center = buffer[node, plane + 1]
            upper, lower = buffer[node, plane + 2], buffer[node, plane]
            z_up, z_down = pltpu.roll(center, size_z - 1, 0), pltpu.roll(center, 1, 0)
            y_up, y_down = pltpu.roll(center, size_y - 1, 1), pltpu.roll(center, 1, 1)
            laplace = (upper + lower) + (z_up + z_down) + (y_up + y_down) - 6.0 * center
            terms.append(factor * laplace)
        transport = (
            floats[0] * (upper - lower) + floats[1] * (y_up - y_down) + floats[2] * (z_up - z_down)
        )
        operated = floats[3] * (diffusion_number * laplace - 0.5 * transport)
        kept = floats[3] * center
        result = []
        for row in range(4):
            total = right[row, plane] + (float(nodes[row]) * operated - kept)
            for column in range(4):
                total = total + float(plan.matrix[row, column]) * terms[column]
            result.append(total)
        return jnp.concatenate(result, axis=0)

    def pair(index, carry):
        plane = 2 * index
        both = jnp.concatenate((driving(plane), driving(plane + 1)), axis=1)
        along_z = table_times(z_high[...], z_low[...], both)
        real, imag = along_z[:rows], along_z[rows:]
        stacked = jnp.concatenate(
            (
                jnp.concatenate((real[:, :size_y], imag[:, :size_y]), axis=1),
                jnp.concatenate((real[:, size_y:], imag[:, size_y:]), axis=1),
            ),
            axis=0,
        )
        along_y = times_table(stacked, y_high[...], y_low[...])
        for offset in range(2):
            part = along_y[offset * rows : (offset + 1) * rows]
            where = pl.ds(plane + offset, rows, stride=block)
            out[0, 0, where, :] = part[:, :size_y]
            out[1, 0, where, :] = part[:, size_y:]
        return carry

    lax.fori_loop(0, block // 2, pair, 0)


def end_spectra(plan, floats, tiles, even, odd):
    size_x, size_y = plan.size_x, plan.size_y
    pairs = []
    for pair in range(2):
        rows = jnp.concatenate([tiles[slab][8 * pair : 8 * pair + 8] for slab in range(plan.slabs)])
        pairs.append(rows * end_scale(floats, rows.shape))
    value = tripled(jnp.concatenate(pairs, axis=1))
    found = [dot(even[...], value), dot(odd[...], value)]
    result = []
    for mode in range(4):
        lanes = slice((mode // 2) * size_y, (mode // 2 + 1) * size_y)
        part = found[mode % 2][:, lanes]
        result.append(times(number(plan.values[mode]), (part[:size_x], part[size_x:])))
    return result


def spread(plan, floats, wave_z, *refs):
    (given, table, f_high, f_low, even, odd, b_high, b_low, j_high, j_low) = refs[:10]
    (local, lf_high, lf_low, lb_high, lb_low, e_high, e_low, end_even, end_odd, out) = refs[10:20]
    (held, sent, x_in, f_send, f_all, growth, c_send, c_all, s_send) = refs[20:29]
    (s_all, d_send, d_all, x_out, y_in) = refs[29:34]
    (x_sems, f_sems, c_sems, s_sems, d_sems, y_sems, in_sems, out_sems) = refs[34:]
    slabs, steps, each = plan.slabs, plan.steps, plan.each
    long, size_x, size_y, own = plan.long, plan.size_x, plan.size_y, plan.own_x
    half, pairs = size_x // 2, steps // 2
    step, slab = lax.axis_index("tm"), lax.axis_index("space")
    parity, place = step % 2, step // 2
    other = (step + 1 - 2 * parity, slab)

    def peer(index):
        return (2 * index + parity, slab)

    def slab_peer(index):
        return (step, index)

    barrier = pltpu.get_barrier_semaphore()
    neighbours = [other]
    neighbours += [slab_peer((slab + shift) % slabs) for shift in range(1, slabs)]
    neighbours += [peer((place + shift) % pairs) for shift in range(1, pairs)]
    for device in neighbours:
        pl.semaphore_signal(barrier, inc=1, device_id=device, device_id_type=MESH)
    pl.semaphore_wait(barrier, len(neighbours))

    def remote(source, target, sems, plane, device):
        return pltpu.make_async_remote_copy(
            src_ref=source,
            dst_ref=target,
            send_sem=sems.at[0, plane],
            recv_sem=sems.at[1, plane],
            device_id=device,
            device_id_type=MESH,
        )

    def await_all(ref, sems, kind, plane):
        pltpu.make_async_copy(ref, ref, sems.at[kind, plane]).wait()

    def fetch(plane):
        return pltpu.make_async_copy(given.at[:, :, :, plane], held.at[plane], in_sems.at[plane])

    def write(plane):
        return pltpu.make_async_copy(held.at[plane], out.at[:, :, :, plane], out_sems.at[plane])

    def fetch_all(plane, carry):
        for index in range(slabs):
            fetch(index * each + plane).start()
        return carry

    lax.fori_loop(0, each, fetch_all, 0)

    def local_mode(index):
        return slice(index * size_y, (index + 1) * size_y)

    def modes_of(plane, index):
        at = index * each + plane
        fetch(at).wait()
        parts = [
            jnp.concatenate(
                [held[at, part, :, mode].reshape(long, size_y) for mode in range(4)], axis=1
            )
            for part in range(2)
        ]
        spectrum = table_times(lf_high[...], lf_low[...], jnp.concatenate(parts, axis=0))
        a_real, a_imag = symbol(local, floats, wave_z, at)
        total, inner = None, []
        shape = (plan.blocks, plan.block, size_y)
        for mode in range(4):
            part = (spectrum[:long, local_mode(mode)], spectrum[long:, local_mode(mode)])
            held[at, 0, :, mode] = part[0].reshape(shape)
            held[at, 1, :, mode] = part[1].reshape(shape)
            part = times(damped_by(a_real, a_imag, complex(plan.values[mode])), part)
            total = part if total is None else plus(total, part)
            inner.append(jnp.concatenate(part, axis=0))
        sent[index, plane, : 2 * long] = table_times(
            lb_high[...], lb_low[...], jnp.concatenate(total, axis=0)
        )
        ends = table_times(e_high[...], e_low[...], jnp.concatenate(inner, axis=1))[:8]
        upper = lax.broadcasted_iota(jnp.int32, (8, size_y), 0) < 4
        for pair in range(2):
            start = 2 * long + 8 * pair
            sent[index, plane, start : start + 8] = jnp.where(
                upper, ends[:, local_mode(2 * pair)], ends[:, local_mode(2 * pair + 1)]
            )

    def modes_stage(plane):
        targets = [(slab + shift) % slabs for shift in range(1, slabs)]
        for target in targets:
            modes_of(plane, target)
        for target in targets:
            remote(
                sent.at[target, plane], x_in.at[slab, plane], x_sems, plane, slab_peer(target)
            ).start()
        modes_of(plane, slab)
        x_in[slab, plane] = sent[slab, plane]

    def solution_of(plane, index):
        at = index * each + plane
        found = table_times(lf_high[...], lf_low[...], y_in[index, plane, : 2 * long])
        before = (found[:long], found[long:])
        start = 2 * long
        ends = jnp.concatenate(
            (y_in[index, plane, start : start + 8], y_in[index, plane, start + 8 :]), axis=1
        )
        value = tripled(ends * end_scale(floats, ends.shape))
        sources = [dot(end_even[...], value), dot(end_odd[...], value)]
        a_real, a_imag = symbol(local, floats, wave_z, at)
        driven = []
        for mode in range(4):
            source = sources[mode % 2][:, local_mode(mode // 2)]
            total = times(number(plan.values[mode]), (source[:long], source[long:]))
            total = plus(total, times(number(plan.weights[mode]), before))
            kept = [held[at, part, :, mode].reshape(long, size_y) for part in range(2)]
            total = plus(total, kept)
            damped = damped_by(a_real, a_imag, complex(plan.values[mode]))
            driven.append(jnp.concatenate(times(damped, total), axis=0))
        back = table_times(lb_high[...], lb_low[...], jnp.concatenate(driven, axis=1))
        shape = (plan.blocks, plan.block, size_y)
        for mode in range(4):
            held[at, 0, :, mode] = back[:long, local_mode(mode)].reshape(shape)
            held[at, 1, :, mode] = back[long:, local_mode(mode)].reshape(shape)

    def solution_stage(plane):
        solution_of(plane, slab)
        write(slab * each + plane).start()
        if slabs > 1:
            await_all(x_out.at[pl.ds(0, slabs - 1), plane], y_sems, 1, plane)
        for shift in range(1, slabs):
            target = (slab + shift) % slabs
            solution_of(plane, target)
            write(target * each + plane).start()

    def symbols(plane, start, count):
        rows = pl.ds(start, count)
        tables = [table[index, rows] for index in range(3)]
        return symbol(tables, floats, wave_z, slab * each + plane)

    def grown(plane, start, count):
        a_real, a_imag = symbols(plane, start, count)
        total = None
        for mode in range(4):
            damped = damped_by(a_real, a_imag, complex(plan.values[mode]))
            term = times(number(plan.weights[mode]), damped)
            total = term if total is None else plus(total, term)
        return total

    def spectrum_stage(plane):
        if slabs > 1:
            await_all(x_in.at[pl.ds(0, slabs - 1), plane], x_sems, 1, plane)
        arrived = [x_in[index, plane] for index in range(slabs)]
        value = jnp.concatenate(
            [part[:long] for part in arrived] + [part[long : 2 * long] for part in arrived], axis=0
        )
        found = table_times(f_high[...], f_low[...], value)
        total = (found[:size_x], found[size_x:])
        sources = end_spectra(plan, floats, [part[2 * long :] for part in arrived], even, odd)
        a_real, a_imag = symbols(plane, 0, size_x)
        for mode in range(4):
            damped = damped_by(a_real, a_imag, complex(plan.values[mode]))
            total = plus(total, times(damped, sources[mode]))
        for index in range(2):
            rows = slice(index * half, (index + 1) * half)
            lower, upper = total[index][:half], total[index][half:]
            f_send[plane, rows] = jnp.where(parity == 0, upper, lower)
            f_all[plane, parity, rows] = jnp.where(parity == 0, lower, upper)
        remote(f_send.at[plane], f_all.at[plane, parity], f_sems, plane, other).start()

    def pair_stage(plane):
        factor = grown(plane, pl.multiple_of(parity * half, half), half)
        growth[plane, :half], growth[plane, half:] = factor
        await_all(f_send.at[plane], f_sems, 1, plane)
        early = (f_all[plane, 0, :half], f_all[plane, 0, half:])
        later = (f_all[plane, 1, :half], f_all[plane, 1, half:])
        total = plus(later, times(factor, early))
        for index in range(pairs):
            rows = slice(index * own, (index + 1) * own)
            c_send[index, plane, :own] = total[0][rows]
            c_send[index, plane, own:] = total[1][rows]
        c_all[place, plane] = c_send[place, plane]
        for shift in range(1, pairs):
            target = (place + shift) % pairs
            remote(
                c_send.at[target, plane], c_all.at[place, plane], c_sems, plane, peer(target)
            ).start()

    def sweep_stage(plane):
        factor = grown(plane, pl.multiple_of(parity * half + place * own, own), own)
        factor = times(factor, factor)
        if pairs > 1:
            await_all(c_all.at[pl.ds(0, pairs - 1), plane], c_sems, 1, plane)
        fields = [(c_all[index, plane, :own], c_all[index, plane, own:]) for index in range(pairs)]
        total, power = fields[0], factor
        for index in range(1, pairs):
            total = plus(fields[index], times(factor, total))
            power = times(factor, power)
        lower = (1.0 - circulant_alpha * power[0], -circulant_alpha * power[1])
        scale = circulant_alpha / (lower[0] * lower[0] + lower[1] * lower[1])
        current = times(total, (lower[0] * scale, -lower[1] * scale))
        for index in range(pairs):
            s_send[index, plane, :own] = current[0]
            s_send[index, plane, own:] = current[1]
            current = plus(fields[index], times(factor, current))
        s_all[place, plane] = s_send[place, plane]
        for shift in range(1, pairs):
            target = (place + shift) % pairs
            remote(
                s_send.at[target, plane], s_all.at[place, plane], s_sems, plane, peer(target)
            ).start()

    def start_stage(plane):
        if pairs > 1:
            await_all(s_all.at[pl.ds(0, pairs - 1), plane], s_sems, 1, plane)
        early = tuple(
            jnp.concatenate([s_all[index, plane, rows] for index in range(pairs)], axis=0)
            for rows in (slice(0, own), slice(own, 2 * own))
        )
        field = (f_all[plane, 0, :half], f_all[plane, 0, half:])
        later = plus(field, times((growth[plane, :half], growth[plane, half:]), early))
        for index in range(2):
            rows = slice(index * half, (index + 1) * half)
            d_send[plane, rows] = jnp.where(parity == 0, later[index], early[index])
            d_all[plane, parity, rows] = jnp.where(parity == 0, early[index], later[index])
        remote(d_send.at[plane], d_all.at[plane, parity], d_sems, plane, other).start()

    def return_stage(plane):
        await_all(d_send.at[plane], d_sems, 1, plane)
        real = jnp.concatenate((d_all[plane, 0, :half], d_all[plane, 1, :half]), axis=0)
        imag = jnp.concatenate((d_all[plane, 0, half:], d_all[plane, 1, half:]), axis=0)
        found = table_times(b_high[...], b_low[...], jnp.concatenate((real, imag), axis=0))
        tiles = [x_in[index, plane, 2 * long :] for index in range(slabs)]
        sources = end_spectra(plan, floats, tiles, even, odd)
        a_real, a_imag = symbols(plane, 0, size_x)
        driven = []
        for mode in range(4):
            damped = damped_by(a_real, a_imag, complex(plan.values[mode]))
            weighted = times(number(plan.weights[mode]), (real, imag))
            driven.append(jnp.concatenate(times(damped, plus(weighted, sources[mode])), axis=0))
        jumps = table_times(j_high[...], j_low[...], jnp.concatenate(driven, axis=1))
        row = lax.broadcasted_iota(jnp.int32, (8, size_y), 0)
        for index in range(slabs):
            first = index * long
            x_out[index, plane, :long] = found[first : first + long]
            x_out[index, plane, long : 2 * long] = found[size_x + first : size_x + first + long]
            above, under = tiles[(index + 1) % slabs], tiles[(index - 1) % slabs]
            for pair in range(2):
                part = slice(8 * pair, 8 * pair + 8)
                here = slice(8 * index, 8 * index + 8)
                local = jnp.where(row % 4 < 2, above[part], under[part]) - tiles[index][part]
                lower = jumps[here, 2 * pair * size_y : (2 * pair + 1) * size_y]
                upper = jumps[here, (2 * pair + 1) * size_y : (2 * pair + 2) * size_y]
                start = 2 * long + 8 * pair
                x_out[index, plane, start : start + 8] = local + jnp.where(row < 4, lower, upper)
        y_in[slab, plane] = x_out[slab, plane]
        for shift in range(1, slabs):
            target = (slab + shift) % slabs
            remote(
                x_out.at[target, plane], y_in.at[slab, plane], y_sems, plane, slab_peer(target)
            ).start()

    stages = (modes_stage, spectrum_stage, pair_stage, sweep_stage)
    stages += (start_stage, return_stage, solution_stage)

    delays = (0, 1, 2, 3, 4, 5, 6)

    def iteration(time, carry):
        for delay in reversed(range(len(stages))):
            plane = time - delays[delay]

            @pl.when(jnp.logical_and(plane >= 0, plane < each))
            def _():
                stages[delay](plane)

        return carry

    lax.fori_loop(0, each + delays[-1], iteration, 0)

    def finish(plane, carry):
        await_all(f_send.at[plane], f_sems, 0, plane)
        await_all(d_send.at[plane], d_sems, 0, plane)
        if pairs > 1:
            await_all(c_send.at[pl.ds(0, pairs - 1), plane], c_sems, 0, plane)
            await_all(s_send.at[pl.ds(0, pairs - 1), plane], s_sems, 0, plane)
        if slabs > 1:
            await_all(x_in.at[pl.ds(0, slabs - 1), plane], x_sems, 0, plane)
            await_all(x_out.at[pl.ds(0, slabs - 1), plane], y_sems, 0, plane)
        for index in range(slabs):
            write(index * each + plane).wait()
        return carry

    lax.fori_loop(0, each, finish, 0)


def leave_kernel(plan, floats, found_in, kept, y_high, y_low, z_high, z_low, z_rest, out):
    block, rows, size_y, size_z = plan.block, plan.rows, plan.size_y, plan.size_z
    most = z_high.shape[1]

    def pair(index, carry):
        plane = 2 * index
        parts = []
        for offset in range(2):
            where = pl.ds(plane + offset, rows, stride=block)
            parts.append(jnp.concatenate((found_in[0, 0, where, :], found_in[1, 0, where, :]), axis=1))
        along_y = times_table(jnp.concatenate(parts, axis=0), y_high[...], y_low[...])
        stacked = jnp.concatenate(
            (
                jnp.concatenate((along_y[:rows, :size_y], along_y[rows:, :size_y]), axis=1),
                jnp.concatenate((along_y[:rows, size_y:], along_y[rows:, size_y:]), axis=1),
            ),
            axis=0,
        )
        found = table_times(z_high[...], z_low[...], stacked[:most])
        if most < 2 * rows:
            found = found + dot(z_rest[...], tripled(stacked[most:]))
        for offset in range(2):
            add = floats[3] * kept[0, plane + offset]
            for node in range(4):
                part = found[node * size_z : (node + 1) * size_z]
                out[node, plane + offset] = part[:, offset * size_y : (offset + 1) * size_y] + add
        return carry

    lax.fori_loop(0, block // 2, pair, 0)


def whole(array):
    zeros = (0,) * array.ndim
    return pl.BlockSpec(array.shape, lambda *at: zeros)


scalars = pl.BlockSpec(memory_space=pltpu.SMEM)


def called(kernel, name, grid, in_specs, out_specs, out_shape, operands, flops=0, scratch=()):
    return pl.pallas_call(
        kernel,
        name=name,
        grid=grid,
        in_specs=in_specs,
        out_specs=out_specs,
        out_shape=out_shape,
        scratch_shapes=list(scratch),
        compiler_params=pltpu.CompilerParams(
            dimension_semantics=("arbitrary",) * len(grid), vmem_limit_bytes=56 * 1024 * 1024
        ),
    )(*operands)


def shaped(*shape):
    return jax.ShapeDtypeStruct(shape, jnp.float32)


def shards(iterate, right_side, diffusivity, velocity):
    steps = lax.axis_size("tm")
    slabs = lax.axis_size("space")
    step = lax.axis_index("tm")
    nodes, long, size_z, size_y = iterate.shape[1:]
    plan = Plan(slabs, steps, long * slabs, size_z, size_y)
    size_x, padded, each = plan.size_x, plan.padded, plan.each
    rows, block, blocks, sent_rows, own = plan.rows, plan.block, plan.blocks, plan.sent, plan.own_x
    iterate, right_side = iterate[0], right_side[0]

    is_last = (step == steps - 1).astype(jnp.float32)
    floats = jnp.concatenate((velocity, is_last[None]))
    wave_z = jnp.asarray(plan.z_symbols())

    forward = [(index, (index + 1) % slabs) for index in range(slabs)]
    backward = [(target, source) for source, target in forward]
    low_halo = lax.ppermute(iterate[:, -1:], "space", forward)
    high_halo = lax.ppermute(iterate[:, :1], "space", backward)

    z_tables = split_constant(plan.z_forward())
    y_tables = split_constant(plan.y_forward())
    tables = list(z_tables + y_tables)
    thick = pl.BlockSpec((4, block, size_z, size_y), lambda at: (0, at, 0, 0))
    thin = (4, 1, size_z, size_y)
    out_block = pl.BlockSpec((2, 1, rows * block, size_y), lambda at: (0, at, 0, 0))
    spectrum = called(
        functools.partial(enter_kernel, plan),
        "enter",
        (blocks,),
        [
            scalars,
            thick,
            pl.BlockSpec(thin, lambda at: (0, jnp.maximum(at * block - 1, 0), 0, 0)),
            pl.BlockSpec(thin, lambda at: (0, jnp.minimum(at * block + block, long - 1), 0, 0)),
            whole(low_halo),
            whole(high_halo),
            thick,
            pl.BlockSpec((block, size_z, size_y), lambda at: (at, 0, 0)),
        ]
        + [whole(table) for table in tables],
        out_block,
        shaped(2, blocks, rows * block, size_y),
        [floats, iterate, iterate, iterate, low_halo, high_halo, right_side, diffusivity] + tables,
        scratch=[pltpu.VMEM((4, block + 2, size_z, size_y), jnp.float32)],
    )

    by_plane = (2, blocks, 4, padded, block, size_y)
    tables = [plan.symbol_tables(size_x)] + list(split_constant(plan.x_forward(size_x)))
    tables += [tripled_constant(matrix) for matrix in plan.jump_sources()]
    tables += list(split_constant(plan.x_backward(size_x)) + split_constant(plan.jumps()))
    tables += [plan.symbol_tables(long)] + list(split_constant(plan.x_forward(long)))
    tables += list(split_constant(plan.x_backward(long)) + split_constant(plan.ends()))
    tables += [tripled_constant(matrix) for matrix in plan.end_sources()]
    half, pairs = size_x // 2, steps // 2
    anywhere = pl.BlockSpec(memory_space=pl.ANY)

    def held(*shape):
        return pltpu.VMEM(shape, jnp.float32)

    halves, parts = (each, 2 * half, size_y), (pairs, each, 2 * own, size_y)
    both = (each, 2, 2 * half, size_y)
    slots = (slabs, each, sent_rows, size_y)
    spectrum = pl.pallas_call(
        functools.partial(spread, plan),
        name="spread",
        in_specs=[scalars, scalars, anywhere]
        + [pl.BlockSpec(memory_space=pltpu.VMEM) for table in tables],
        out_specs=anywhere,
        out_shape=shaped(*by_plane),
        scratch_shapes=[
            held(padded, 2, blocks, 4, block, size_y),
            held(*slots),
            held(*slots),
            held(*halves),
            held(*both),
            held(*halves),
            held(*parts),
            held(*parts),
            held(*parts),
            held(*parts),
            held(*halves),
            held(*both),
            held(*slots),
            held(*slots),
        ]
        + [pltpu.SemaphoreType.DMA((2, each))] * 6
        + [pltpu.SemaphoreType.DMA((padded,))] * 2,
        compiler_params=pltpu.CompilerParams(
            collective_id=0, has_side_effects=True, vmem_limit_bytes=56 * 1024 * 1024
        ),
    )(floats, wave_z, spectrum.reshape(by_plane), *tables)

    z_backward = plan.z_backward()
    most = min(256, 2 * rows)
    z_tables = split_constant(z_backward[:, :most])
    rest = z_backward[:, most:] if most < 2 * rows else z_backward[:, :16]
    tables = list(split_constant(plan.y_backward()) + z_tables) + [tripled_constant(rest)]
    result = called(
        functools.partial(leave_kernel, plan),
        "leave",
        (blocks,),
        [
            scalars,
            out_block,
            pl.BlockSpec((1, block, size_z, size_y), lambda at: (3, at, 0, 0)),
        ]
        + [whole(table) for table in tables],
        thick,
        shaped(4, long, size_z, size_y),
        [
            floats,
            spectrum.reshape(2, blocks, rows * block, size_y),
            iterate,
        ]
        + tables,
    )
    return result[None]


def solution(mesh):
    placed = (
        P("tm", None, "space", None, None),
        P("tm", None, "space", None, None),
        P("space", None, None),
        P(),
    )
    return jax.shard_map(
        shards,
        mesh=mesh,
        in_specs=placed,
        out_specs=P("tm", None, "space", None, None),
        check_vma=False,
    )
```

```python
import functools
import math

import jax
import jax.numpy as jnp
import numpy as np
from jax import lax
from jax.experimental import pallas as pl
from jax.experimental.pallas import tpu as pltpu
from jax.sharding import PartitionSpec as P

diffusion_number = 16.0
circulant_alpha = 0.1
MESH = pl.DeviceIdType.MESH


def collocation_matrix():
    radau_nodes = [0.08858795951270394, 0.4094668644407347, 0.7876594617608471, 1.0]
    matrix = [[0.0] * 4 for row_index in range(4)]
    for column_index in range(4):
        coefficients = [1.0]
        for other_index in range(4):
            if other_index != column_index:
                scale_value = 1.0 / (radau_nodes[column_index] - radau_nodes[other_index])
                shifted = [0.0] + [value * scale_value for value in coefficients]
                lowered = [
                    -radau_nodes[other_index] * scale_value * value for value in coefficients
                ] + [0.0]
                coefficients = [
                    left_value + right_value for left_value, right_value in zip(shifted, lowered)
                ]
        for row_index in range(4):
            total = 0.0
            for power_index in range(len(coefficients)):
                total = total + coefficients[power_index] * radau_nodes[row_index] ** (
                    power_index + 1
                ) / (power_index + 1)
            matrix[row_index][column_index] = total
    return matrix


def solve_system(matrix, target):
    count = len(target)
    rows_list = [list(matrix[row_index]) + [target[row_index]] for row_index in range(count)]
    for column in range(count):
        best_row = column
        for candidate in range(column + 1, count):
            if abs(rows_list[candidate][column]) > abs(rows_list[best_row][column]):
                best_row = candidate
        saved_row = rows_list[column]
        rows_list[column] = rows_list[best_row]
        rows_list[best_row] = saved_row
        leader = rows_list[column][column]
        for other_row in range(count):
            if other_row != column:
                factor = rows_list[other_row][column] / leader
                rows_list[other_row] = [
                    left_value - factor * right_value
                    for left_value, right_value in zip(rows_list[other_row], rows_list[column])
                ]
    return [
        rows_list[row_index][count] / rows_list[row_index][row_index] for row_index in range(count)
    ]


def node_basis():
    matrix = collocation_matrix()
    helper = [[0.0] * 4 for row_index in range(4)]
    coefficients = [0.0, 0.0, 0.0, 0.0, 1.0]
    for order in range(1, 5):
        product = [
            [
                sum((matrix[row_index][inner] * helper[inner][column] for inner in range(4)))
                for column in range(4)
            ]
            for row_index in range(4)
        ]
        for row_index in range(4):
            product[row_index][row_index] = product[row_index][row_index] + coefficients[5 - order]
        helper = product
        trace_value = sum(
            (
                sum((matrix[row_index][inner] * helper[inner][row_index] for inner in range(4)))
                for row_index in range(4)
            )
        )
        coefficients[4 - order] = -trace_value / order
    roots_list = [(0.4 + 0.9j) ** power_index for power_index in range(4)]
    for sweep in range(400):
        for root_index in range(4):
            current = roots_list[root_index]
            numer = 0.0
            for power_index in range(4, -1, -1):
                numer = numer * current + coefficients[power_index]
            denom = 1.0
            for other_index in range(4):
                if other_index != root_index:
                    denom = denom * (current - roots_list[other_index])
            roots_list[root_index] = current - numer / denom
    vectors = [[0.0] * 4 for row_index in range(4)]
    for root_index in range(4):
        shifted = [
            [
                matrix[row_index][column] - (roots_list[root_index] if row_index == column else 0.0)
                for column in range(3)
            ]
            for row_index in range(3)
        ]
        target = [-matrix[row_index][3] for row_index in range(3)]
        parts = solve_system(shifted, target) + [1.0 + 0j]
        for row_index in range(4):
            vectors[row_index][root_index] = parts[row_index]
    inverse = [[0.0] * 4 for row_index in range(4)]
    for column in range(4):
        unit = [1.0 if row_index == column else 0.0 for row_index in range(4)]
        parts = solve_system(vectors, unit)
        for row_index in range(4):
            inverse[row_index][column] = parts[row_index]
    weights = [sum((inverse[row_index][column] for column in range(4))) for row_index in range(4)]
    return (roots_list, vectors, inverse, weights)


def split_constant(matrix):
    high = matrix.astype(jnp.bfloat16)
    low = (matrix - high.astype(np.float64)).astype(jnp.bfloat16)
    return high, low


def split(value):
    high = value.astype(jnp.bfloat16)
    low = (value - high.astype(jnp.float32)).astype(jnp.bfloat16)
    return high, low


def dot(left, right):
    return jnp.dot(left, right, preferred_element_type=jnp.float32)


def table_times(high, low, value):
    value_high, value_low = split(value)
    return dot(high, value_high) + dot(high, value_low) + dot(low, value_high)


def times_table(value, high, low):
    value_high, value_low = split(value)
    return dot(value_high, high) + dot(value_low, high) + dot(value_high, low)


def tripled(value):
    high = value.astype(jnp.bfloat16).astype(jnp.float32)
    return jnp.concatenate((high, value - high, high), axis=0).astype(jnp.bfloat16)


def tripled_constant(matrix):
    high, low = split_constant(matrix)
    return np.concatenate((high, high, low), axis=1)


def complex_block(matrix):
    return np.block([[matrix.real, -matrix.imag], [matrix.imag, matrix.real]])


def fourier(rows, columns, length, sign):
    phases = np.outer(rows, columns) % length
    return np.exp(sign * 2j * np.pi * phases / length)


class Plan:
    def __init__(self, slabs, steps, size_x, size_z, size_y):
        self.slabs, self.steps = slabs, steps
        self.size_x, self.size_z, self.size_y = size_x, size_z, size_y
        self.long = long = size_x // slabs
        self.planes = size_z // 2 + 1
        each = -(-self.planes // slabs)
        while (each * slabs) % 2:
            each += 1
        self.each = each
        self.padded = each * slabs
        self.rows = 4 * self.padded
        self.block = 8
        self.blocks = long // self.block
        self.own_x = size_x // steps
        self.sent = 2 * long + 16
        self.values, self.vectors, self.inverse, self.weights = node_basis()
        self.matrix = np.array(collocation_matrix())

    def symbol_tables(self, length):
        theta_x = 2.0 * np.pi * np.arange(length)[:, None] / length
        theta_y = 2.0 * np.pi * np.arange(self.size_y)[None, :] / self.size_y
        real = diffusion_number * (2.0 * np.cos(theta_x) + 2.0 * np.cos(theta_y) - 4.0)
        ones = np.ones_like(real)
        return np.stack((real, np.sin(theta_x) * ones, np.sin(theta_y) * ones)).astype(np.float32)

    def z_symbols(self):
        theta = 2.0 * np.pi * np.arange(self.padded) / self.size_z
        return np.stack((diffusion_number * (2.0 * np.cos(theta) - 2.0), np.sin(theta))).astype(
            np.float32
        )

    def z_forward(self):
        wave = fourier(np.arange(self.padded), np.arange(self.size_z), self.size_z, -1.0)
        wave[self.planes :] = 0.0
        full = np.einsum("mn,kz->mknz", np.array(self.inverse), wave)
        full = full.reshape(self.rows, 4 * self.size_z)
        return np.concatenate((full.real, full.imag), axis=0)

    def z_backward(self):
        wave = fourier(np.arange(self.size_z), np.arange(self.padded), self.size_z, 1.0)
        weight = np.full(self.padded, 2.0)
        weight[0] = 1.0
        weight[self.planes - 1] = 1.0
        weight[self.planes :] = 0.0
        wave = wave * weight / self.size_z
        full = np.einsum("nm,zk->nzmk", np.array(self.vectors), wave)
        full = full.reshape(4 * self.size_z, self.rows)
        return np.concatenate((full.real, -full.imag), axis=1)

    def y_forward(self):
        span = np.arange(self.size_y)
        return complex_block(fourier(span, span, self.size_y, -1.0)).T

    def y_backward(self):
        span = np.arange(self.size_y)
        return complex_block(fourier(span, span, self.size_y, 1.0)).T / self.size_y

    def x_forward(self, length):
        span = np.arange(length)
        return complex_block(fourier(span, span, length, -1.0))

    def x_backward(self, length):
        span = np.arange(length)
        return complex_block(fourier(span, span, length, 1.0)) / length

    def ends(self):
        points = np.array([0, self.long - 1])
        wave = fourier(points, np.arange(self.long), self.long, 1.0) / self.long
        full = complex_block(wave)[[0, 2, 1, 3]]
        return np.concatenate((full, full, full, full), axis=0)

    def jump_sources(self):
        wave = np.arange(self.size_x)
        even = []
        for slab in range(self.slabs):
            start = slab * self.long

            def phase(point):
                return fourier(wave, np.array([point % self.size_x]), self.size_x, -1.0)[:, 0]

            first = phase(start - 1) - phase(start + self.long - 1)
            last = phase(start + self.long) - phase(start)
            even.append(np.stack((first, 1j * first, last, 1j * last), axis=1))
        return self.by_parity(even)

    def by_parity(self, blocks):
        zero = np.zeros_like(blocks[0])
        even = np.concatenate([part for block in blocks for part in (block, zero)], axis=1)
        odd = np.concatenate([part for block in blocks for part in (zero, block)], axis=1)
        return [np.concatenate((full.real, full.imag), axis=0) for full in (even, odd)]

    def end_sources(self):
        wave = np.arange(self.long)
        upper = fourier(wave, np.array([1]), self.long, 1.0)[:, 0]
        lower = np.ones_like(upper)
        return self.by_parity([np.stack((upper, 1j * upper, lower, 1j * lower), axis=1)])

    def jumps(self):
        wave = np.arange(self.size_x)
        rows = []
        for slab in range(self.slabs):
            start = slab * self.long
            points = np.array([start + self.long, start, start - 1, start + self.long - 1])
            value = fourier(points % self.size_x, wave, self.size_x, 1.0) / self.size_x
            upper, lower = value[0] - value[1], value[2] - value[3]
            full = complex_block(np.stack((upper, lower)))[[0, 2, 1, 3]]
            rows += [full, full]
        return np.concatenate(rows, axis=0)


def damped_by(real, imag, value):
    lower_real = 1.0 - (real * value.real - imag * value.imag)
    lower_imag = real * value.imag + imag * value.real
    scale = 1.0 / (lower_real * lower_real + lower_imag * lower_imag)
    return lower_real * scale, lower_imag * scale


def symbol(table, floats, wave_z, plane):
    real = table[0] + wave_z[0, plane]
    imag = -(floats[0] * table[1] + floats[1] * table[2] + floats[2] * wave_z[1, plane])
    return real, imag


def times(left, right):
    return (left[0] * right[0] - left[1] * right[1], left[0] * right[1] + left[1] * right[0])


def plus(left, right):
    return (left[0] + right[0], left[1] + right[1])


def number(value):
    value = complex(value)
    return (value.real, value.imag)


def end_scale(floats, shape):
    row = lax.broadcasted_iota(jnp.int32, shape, 0) % 4
    upper = diffusion_number - 0.5 * floats[0]
    lower = diffusion_number + 0.5 * floats[0]
    return jnp.where(row < 2, upper, lower)


def enter_kernel(plan, floats, it, below, above, right, diff, field, *refs):
    z_high, z_low, y_high, y_low, out, buffer, halo, sends, receives = refs
    block, rows, size_y, slabs = plan.block, plan.rows, plan.size_y, plan.slabs
    count = plan.blocks
    turn = pl.program_id(0)
    at = (turn + 1) % count
    step, slab = lax.axis_index("tm"), lax.axis_index("space")
    upper_slab, lower_slab = (step, (slab + 1) % slabs), (step, (slab + slabs - 1) % slabs)

    def edge(index):
        plane = (plan.long - 1, 0)[index]
        return pltpu.make_async_remote_copy(
            src_ref=field.at[:, pl.ds(plane, 1)],
            dst_ref=halo.at[index],
            send_sem=sends.at[index],
            recv_sem=receives.at[index],
            device_id=(upper_slab, lower_slab)[index],
            device_id_type=MESH,
        )

    @pl.when(turn == 0)
    def _():
        barrier = pltpu.get_barrier_semaphore()
        for device in (upper_slab, lower_slab):
            pl.semaphore_signal(barrier, inc=1, device_id=device, device_id_type=MESH)
        pl.semaphore_wait(barrier, 2)
        for index in range(2):
            edge(index).start()

    @pl.when(turn == max(count - 2, 0))
    def _():
        for index in range(2):
            edge(index).wait()

    buffer[:, 1 : block + 1] = it[...]
    buffer[:, 0:1] = below[...]
    buffer[:, block + 1 :] = above[...]

    @pl.when(at == 0)
    def _():
        buffer[:, 0:1] = halo[0]

    @pl.when(at == count - 1)
    def _():
        buffer[:, block + 1 :] = halo[1]

    nodes = plan.matrix.sum(axis=1)
    size_z = plan.size_z

    def driving(plane):
        factor = diffusion_number * (diff[plane] - 1.0)
        terms = []
        for node in range(4):
            center = buffer[node, plane + 1]
            upper, lower = buffer[node, plane + 2], buffer[node, plane]
            z_up, z_down = pltpu.roll(center, size_z - 1, 0), pltpu.roll(center, 1, 0)
            y_up, y_down = pltpu.roll(center, size_y - 1, 1), pltpu.roll(center, 1, 1)
            laplace = (upper + lower) + (z_up + z_down) + (y_up + y_down) - 6.0 * center
            terms.append(factor * laplace)
        transport = (
            floats[0] * (upper - lower) + floats[1] * (y_up - y_down) + floats[2] * (z_up - z_down)
        )
        operated = floats[3] * (diffusion_number * laplace - 0.5 * transport)
        kept = floats[3] * center
        result = []
        for row in range(4):
            total = right[row, plane] + (float(nodes[row]) * operated - kept)
            for column in range(4):
                total = total + float(plan.matrix[row, column]) * terms[column]
            result.append(total)
        return jnp.concatenate(result, axis=0)

    def pair(index, carry):
        plane = 2 * index
        both = jnp.concatenate((driving(plane), driving(plane + 1)), axis=1)
        along_z = table_times(z_high[...], z_low[...], both)
        real, imag = along_z[:rows], along_z[rows:]
        stacked = jnp.concatenate(
            (
                jnp.concatenate((real[:, :size_y], imag[:, :size_y]), axis=1),
                jnp.concatenate((real[:, size_y:], imag[:, size_y:]), axis=1),
            ),
            axis=0,
        )
        along_y = times_table(stacked, y_high[...], y_low[...])
        for offset in range(2):
            part = along_y[offset * rows : (offset + 1) * rows]
            where = pl.ds(plane + offset, rows, stride=block)
            out[0, 0, where, :] = part[:, :size_y]
            out[1, 0, where, :] = part[:, size_y:]
        return carry

    lax.fori_loop(0, block // 2, pair, 0, unroll=4)


def end_spectra(plan, floats, tiles, even, odd):
    size_x, size_y = plan.size_x, plan.size_y
    pairs = []
    for pair in range(2):
        rows = jnp.concatenate([tiles[slab][8 * pair : 8 * pair + 8] for slab in range(plan.slabs)])
        pairs.append(rows * end_scale(floats, rows.shape))
    value = tripled(jnp.concatenate(pairs, axis=1))
    found = [dot(even[...], value), dot(odd[...], value)]
    result = []
    for mode in range(4):
        lanes = slice((mode // 2) * size_y, (mode // 2 + 1) * size_y)
        part = found[mode % 2][:, lanes]
        result.append(times(number(plan.values[mode]), (part[:size_x], part[size_x:])))
    return result


def spread(plan, floats, wave_z, *refs):
    (given, table, f_high, f_low, even, odd, b_high, b_low, j_high, j_low) = refs[:10]
    (local, lf_high, lf_low, lb_high, lb_low, e_high, e_low, end_even, end_odd, out) = refs[10:20]
    (held, sent, x_in, f_send, f_all, growth, c_send, c_all, s_send) = refs[20:29]
    (s_all, d_send, d_all, x_out, y_in) = refs[29:34]
    (x_sems, f_sems, c_sems, s_sems, d_sems, y_sems, in_sems, out_sems) = refs[34:]
    slabs, steps, each = plan.slabs, plan.steps, plan.each
    long, size_x, size_y, own = plan.long, plan.size_x, plan.size_y, plan.own_x
    half, pairs = size_x // 2, steps // 2
    step, slab = lax.axis_index("tm"), lax.axis_index("space")
    parity, place = step % 2, step // 2
    other = (step + 1 - 2 * parity, slab)

    def peer(index):
        return (2 * index + parity, slab)

    def slab_peer(index):
        return (step, index)

    barrier = pltpu.get_barrier_semaphore()
    neighbours = [other]
    neighbours += [slab_peer((slab + shift) % slabs) for shift in range(1, slabs)]
    neighbours += [peer((place + shift) % pairs) for shift in range(1, pairs)]
    for device in neighbours:
        pl.semaphore_signal(barrier, inc=1, device_id=device, device_id_type=MESH)
    pl.semaphore_wait(barrier, len(neighbours))

    def remote(source, target, sems, plane, device):
        return pltpu.make_async_remote_copy(
            src_ref=source,
            dst_ref=target,
            send_sem=sems.at[0, plane],
            recv_sem=sems.at[1, plane],
            device_id=device,
            device_id_type=MESH,
        )

    def await_all(ref, sems, kind, plane):
        pltpu.make_async_copy(ref, ref, sems.at[kind, plane]).wait()

    def fetch(plane):
        return pltpu.make_async_copy(given.at[:, :, :, plane], held.at[plane], in_sems.at[plane])

    def write(plane):
        return pltpu.make_async_copy(held.at[plane], out.at[:, :, :, plane], out_sems.at[plane])

    def fetch_all(plane, carry):
        for index in range(slabs):
            fetch(index * each + plane).start()
        return carry

    lax.fori_loop(0, each, fetch_all, 0)

    def local_mode(index):
        return slice(index * size_y, (index + 1) * size_y)

    def spectrum_of(plane, index):
        at = index * each + plane
        parts = [
            jnp.concatenate(
                [held[at, part, :, mode].reshape(long, size_y) for mode in range(4)], axis=1
            )
            for part in range(2)
        ]
        return table_times(lf_high[...], lf_low[...], jnp.concatenate(parts, axis=0))

    def modes_of(plane, index, spectrum):
        at = index * each + plane
        a_real, a_imag = symbol(local, floats, wave_z, at)
        total, inner = None, []
        shape = (plan.blocks, plan.block, size_y)
        for mode in range(4):
            part = (spectrum[:long, local_mode(mode)], spectrum[long:, local_mode(mode)])
            held[at, 0, :, mode] = part[0].reshape(shape)
            held[at, 1, :, mode] = part[1].reshape(shape)
            part = times(damped_by(a_real, a_imag, complex(plan.values[mode])), part)
            total = part if total is None else plus(total, part)
            inner.append(jnp.concatenate(part, axis=0))
        sent[index, plane, : 2 * long] = table_times(
            lb_high[...], lb_low[...], jnp.concatenate(total, axis=0)
        )
        ends = table_times(e_high[...], e_low[...], jnp.concatenate(inner, axis=1))[:8]
        upper = lax.broadcasted_iota(jnp.int32, (8, size_y), 0) < 4
        for pair in range(2):
            start = 2 * long + 8 * pair
            sent[index, plane, start : start + 8] = jnp.where(
                upper, ends[:, local_mode(2 * pair)], ends[:, local_mode(2 * pair + 1)]
            )

    def modes_stage(plane):
        targets = [(slab + shift) % slabs for shift in range(1, slabs)]
        for index in range(slabs):
            fetch(index * each + plane).wait()
        spectra = [spectrum_of(plane, index) for index in range(slabs)]
        for index in range(slabs):
            modes_of(plane, index, spectra[index])
        x_in[slab, plane] = sent[slab, plane]
        for target in targets:
            remote(
                sent.at[target, plane], x_in.at[slab, plane], x_sems, plane, slab_peer(target)
            ).start()

    def solution_of(plane, index):
        at = index * each + plane
        found = table_times(lf_high[...], lf_low[...], y_in[index, plane, : 2 * long])
        before = (found[:long], found[long:])
        start = 2 * long
        ends = jnp.concatenate(
            (y_in[index, plane, start : start + 8], y_in[index, plane, start + 8 :]), axis=1
        )
        value = tripled(ends * end_scale(floats, ends.shape))
        sources = [dot(end_even[...], value), dot(end_odd[...], value)]
        a_real, a_imag = symbol(local, floats, wave_z, at)
        driven = []
        for mode in range(4):
            source = sources[mode % 2][:, local_mode(mode // 2)]
            total = times(number(plan.values[mode]), (source[:long], source[long:]))
            total = plus(total, times(number(plan.weights[mode]), before))
            kept = [held[at, part, :, mode].reshape(long, size_y) for part in range(2)]
            total = plus(total, kept)
            damped = damped_by(a_real, a_imag, complex(plan.values[mode]))
            driven.append(jnp.concatenate(times(damped, total), axis=0))
        return jnp.concatenate(driven, axis=1)

    def keep_solution(plane, index, driven):
        at = index * each + plane
        back = table_times(lb_high[...], lb_low[...], driven)
        shape = (plan.blocks, plan.block, size_y)
        for mode in range(4):
            held[at, 0, :, mode] = back[:long, local_mode(mode)].reshape(shape)
            held[at, 1, :, mode] = back[long:, local_mode(mode)].reshape(shape)

    def solution_stage(plane):
        if slabs > 1:
            await_all(x_out.at[pl.ds(0, slabs - 1), plane], y_sems, 1, plane)
        driven = [solution_of(plane, index) for index in range(slabs)]
        for index in range(slabs):
            keep_solution(plane, index, driven[index])
        for index in range(slabs):
            write(index * each + plane).start()

    def symbols(plane, start, count):
        rows = pl.ds(start, count)
        tables = [table[index, rows] for index in range(3)]
        return symbol(tables, floats, wave_z, slab * each + plane)

    def grown(plane, start, count):
        a_real, a_imag = symbols(plane, start, count)
        total = None
        for mode in range(4):
            damped = damped_by(a_real, a_imag, complex(plan.values[mode]))
            term = times(number(plan.weights[mode]), damped)
            total = term if total is None else plus(total, term)
        return total

    def spectrum_stage(plane):
        if slabs > 1:
            await_all(x_in.at[pl.ds(0, slabs - 1), plane], x_sems, 1, plane)
        arrived = [x_in[index, plane] for index in range(slabs)]
        value = jnp.concatenate(
            [part[:long] for part in arrived] + [part[long : 2 * long] for part in arrived], axis=0
        )
        found = table_times(f_high[...], f_low[...], value)
        total = (found[:size_x], found[size_x:])
        sources = end_spectra(plan, floats, [part[2 * long :] for part in arrived], even, odd)
        a_real, a_imag = symbols(plane, 0, size_x)
        for mode in range(4):
            damped = damped_by(a_real, a_imag, complex(plan.values[mode]))
            total = plus(total, times(damped, sources[mode]))
        for index in range(2):
            rows = slice(index * half, (index + 1) * half)
            lower, upper = total[index][:half], total[index][half:]
            f_send[plane, rows] = jnp.where(parity == 0, upper, lower)
            f_all[plane, parity, rows] = jnp.where(parity == 0, lower, upper)
        remote(f_send.at[plane], f_all.at[plane, parity], f_sems, plane, other).start()

    def pair_stage(plane):
        factor = grown(plane, pl.multiple_of(parity * half, half), half)
        growth[plane, :half], growth[plane, half:] = factor
        await_all(f_send.at[plane], f_sems, 1, plane)
        early = (f_all[plane, 0, :half], f_all[plane, 0, half:])
        later = (f_all[plane, 1, :half], f_all[plane, 1, half:])
        total = plus(later, times(factor, early))
        for index in range(pairs):
            rows = slice(index * own, (index + 1) * own)
            c_send[index, plane, :own] = total[0][rows]
            c_send[index, plane, own:] = total[1][rows]
        c_all[place, plane] = c_send[place, plane]
        for shift in range(1, pairs):
            target = (place + shift) % pairs
            remote(
                c_send.at[target, plane], c_all.at[place, plane], c_sems, plane, peer(target)
            ).start()

    def sweep_stage(plane):
        factor = grown(plane, pl.multiple_of(parity * half + place * own, own), own)
        factor = times(factor, factor)
        if pairs > 1:
            await_all(c_all.at[pl.ds(0, pairs - 1), plane], c_sems, 1, plane)
        fields = [(c_all[index, plane, :own], c_all[index, plane, own:]) for index in range(pairs)]
        total, power = fields[0], factor
        for index in range(1, pairs):
            total = plus(fields[index], times(factor, total))
            power = times(factor, power)
        lower = (1.0 - circulant_alpha * power[0], -circulant_alpha * power[1])
        scale = circulant_alpha / (lower[0] * lower[0] + lower[1] * lower[1])
        current = times(total, (lower[0] * scale, -lower[1] * scale))
        for index in range(pairs):
            s_send[index, plane, :own] = current[0]
            s_send[index, plane, own:] = current[1]
            current = plus(fields[index], times(factor, current))
        s_all[place, plane] = s_send[place, plane]
        for shift in range(1, pairs):
            target = (place + shift) % pairs
            remote(
                s_send.at[target, plane], s_all.at[place, plane], s_sems, plane, peer(target)
            ).start()

    def start_stage(plane):
        if pairs > 1:
            await_all(s_all.at[pl.ds(0, pairs - 1), plane], s_sems, 1, plane)
        early = tuple(
            jnp.concatenate([s_all[index, plane, rows] for index in range(pairs)], axis=0)
            for rows in (slice(0, own), slice(own, 2 * own))
        )
        field = (f_all[plane, 0, :half], f_all[plane, 0, half:])
        later = plus(field, times((growth[plane, :half], growth[plane, half:]), early))
        for index in range(2):
            rows = slice(index * half, (index + 1) * half)
            d_send[plane, rows] = jnp.where(parity == 0, later[index], early[index])
            d_all[plane, parity, rows] = jnp.where(parity == 0, early[index], later[index])
        remote(d_send.at[plane], d_all.at[plane, parity], d_sems, plane, other).start()

    def return_stage(plane):
        await_all(d_send.at[plane], d_sems, 1, plane)
        real = jnp.concatenate((d_all[plane, 0, :half], d_all[plane, 1, :half]), axis=0)
        imag = jnp.concatenate((d_all[plane, 0, half:], d_all[plane, 1, half:]), axis=0)
        found = table_times(b_high[...], b_low[...], jnp.concatenate((real, imag), axis=0))
        tiles = [x_in[index, plane, 2 * long :] for index in range(slabs)]
        sources = end_spectra(plan, floats, tiles, even, odd)
        a_real, a_imag = symbols(plane, 0, size_x)
        driven = []
        for mode in range(4):
            damped = damped_by(a_real, a_imag, complex(plan.values[mode]))
            weighted = times(number(plan.weights[mode]), (real, imag))
            driven.append(jnp.concatenate(times(damped, plus(weighted, sources[mode])), axis=0))
        jumps = table_times(j_high[...], j_low[...], jnp.concatenate(driven, axis=1))
        row = lax.broadcasted_iota(jnp.int32, (8, size_y), 0)
        for index in range(slabs):
            first = index * long
            x_out[index, plane, :long] = found[first : first + long]
            x_out[index, plane, long : 2 * long] = found[size_x + first : size_x + first + long]
            above, under = tiles[(index + 1) % slabs], tiles[(index - 1) % slabs]
            for pair in range(2):
                part = slice(8 * pair, 8 * pair + 8)
                here = slice(8 * index, 8 * index + 8)
                local = jnp.where(row % 4 < 2, above[part], under[part]) - tiles[index][part]
                lower = jumps[here, 2 * pair * size_y : (2 * pair + 1) * size_y]
                upper = jumps[here, (2 * pair + 1) * size_y : (2 * pair + 2) * size_y]
                start = 2 * long + 8 * pair
                x_out[index, plane, start : start + 8] = local + jnp.where(row < 4, lower, upper)
        y_in[slab, plane] = x_out[slab, plane]
        for shift in range(1, slabs):
            target = (slab + shift) % slabs
            remote(
                x_out.at[target, plane], y_in.at[slab, plane], y_sems, plane, slab_peer(target)
            ).start()

    stages = (modes_stage, spectrum_stage, pair_stage, sweep_stage)
    stages += (start_stage, return_stage, solution_stage)

    delays = (0, 1, 2, 3, 4, 5, 6)

    def iteration(time, carry):
        for delay in range(len(stages)):
            plane = time - delays[delay]

            @pl.when(jnp.logical_and(plane >= 0, plane < each))
            def _():
                stages[delay](plane)

        return carry

    lax.fori_loop(0, each + delays[-1], iteration, 0)

    def finish(plane, carry):
        await_all(f_send.at[plane], f_sems, 0, plane)
        await_all(d_send.at[plane], d_sems, 0, plane)
        if pairs > 1:
            await_all(c_send.at[pl.ds(0, pairs - 1), plane], c_sems, 0, plane)
            await_all(s_send.at[pl.ds(0, pairs - 1), plane], s_sems, 0, plane)
        if slabs > 1:
            await_all(x_in.at[pl.ds(0, slabs - 1), plane], x_sems, 0, plane)
            await_all(x_out.at[pl.ds(0, slabs - 1), plane], y_sems, 0, plane)
        for index in range(slabs):
            write(index * each + plane).wait()
        return carry

    lax.fori_loop(0, each, finish, 0)


def leave_kernel(plan, floats, found_in, kept, y_high, y_low, z_high, z_low, z_rest, out):
    block, rows, size_y, size_z = plan.block, plan.rows, plan.size_y, plan.size_z
    most = z_high.shape[1]

    def pair(index, carry):
        plane = 2 * index
        parts = []
        for offset in range(2):
            where = pl.ds(plane + offset, rows, stride=block)
            parts.append(jnp.concatenate((found_in[0, 0, where, :], found_in[1, 0, where, :]), axis=1))
        along_y = times_table(jnp.concatenate(parts, axis=0), y_high[...], y_low[...])
        stacked = jnp.concatenate(
            (
                jnp.concatenate((along_y[:rows, :size_y], along_y[rows:, :size_y]), axis=1),
                jnp.concatenate((along_y[:rows, size_y:], along_y[rows:, size_y:]), axis=1),
            ),
            axis=0,
        )
        found = table_times(z_high[...], z_low[...], stacked[:most])
        if most < 2 * rows:
            found = found + dot(z_rest[...], tripled(stacked[most:]))
        for offset in range(2):
            add = floats[3] * kept[0, plane + offset]
            for node in range(4):
                part = found[node * size_z : (node + 1) * size_z]
                out[node, plane + offset] = part[:, offset * size_y : (offset + 1) * size_y] + add
        return carry

    lax.fori_loop(0, block // 2, pair, 0, unroll=4)


def whole(array):
    zeros = (0,) * array.ndim
    return pl.BlockSpec(array.shape, lambda *at: zeros)


scalars = pl.BlockSpec(memory_space=pltpu.SMEM)


def called(kernel, name, grid, in_specs, out_specs, out_shape, operands, scratch=(), collective=None):
    return pl.pallas_call(
        kernel,
        name=name,
        grid=grid,
        in_specs=in_specs,
        out_specs=out_specs,
        out_shape=out_shape,
        scratch_shapes=list(scratch),
        compiler_params=pltpu.CompilerParams(
            dimension_semantics=("arbitrary",) * len(grid),
            vmem_limit_bytes=56 * 1024 * 1024,
            collective_id=collective,
            has_side_effects=collective is not None,
        ),
    )(*operands)


def shaped(*shape):
    return jax.ShapeDtypeStruct(shape, jnp.float32)


def shards(iterate, right_side, diffusivity, velocity):
    steps = lax.axis_size("tm")
    slabs = lax.axis_size("space")
    step = lax.axis_index("tm")
    nodes, long, size_z, size_y = iterate.shape[1:]
    plan = Plan(slabs, steps, long * slabs, size_z, size_y)
    size_x, padded, each = plan.size_x, plan.padded, plan.each
    rows, block, blocks, sent_rows, own = plan.rows, plan.block, plan.blocks, plan.sent, plan.own_x
    iterate, right_side = iterate[0], right_side[0]

    is_last = (step == steps - 1).astype(jnp.float32)
    floats = jnp.concatenate((velocity, is_last[None]))
    wave_z = jnp.asarray(plan.z_symbols())

    z_tables = split_constant(plan.z_forward())
    y_tables = split_constant(plan.y_forward())
    tables = list(z_tables + y_tables)
    thin = (4, 1, size_z, size_y)
    anywhere = pl.BlockSpec(memory_space=pl.ANY)

    def turned(at):
        return (at + 1) % blocks

    spectrum = called(
        functools.partial(enter_kernel, plan),
        "enter",
        (blocks,),
        [
            scalars,
            pl.BlockSpec((4, block, size_z, size_y), lambda at: (0, turned(at), 0, 0)),
            pl.BlockSpec(thin, lambda at: (0, jnp.maximum(turned(at) * block - 1, 0), 0, 0)),
            pl.BlockSpec(
                thin, lambda at: (0, jnp.minimum(turned(at) * block + block, long - 1), 0, 0)
            ),
            pl.BlockSpec((4, block, size_z, size_y), lambda at: (0, turned(at), 0, 0)),
            pl.BlockSpec((block, size_z, size_y), lambda at: (turned(at), 0, 0)),
            anywhere,
        ]
        + [whole(table) for table in tables],
        pl.BlockSpec((2, 1, rows * block, size_y), lambda at: (0, turned(at), 0, 0)),
        shaped(2, blocks, rows * block, size_y),
        [floats, iterate, iterate, iterate, right_side, diffusivity, iterate] + tables,
        scratch=[
            pltpu.VMEM((4, block + 2, size_z, size_y), jnp.float32),
            pltpu.VMEM((2,) + thin, jnp.float32),
            pltpu.SemaphoreType.DMA((2,)),
            pltpu.SemaphoreType.DMA((2,)),
        ],
        collective=1,
    )

    by_plane = (2, blocks, 4, padded, block, size_y)
    tables = [plan.symbol_tables(size_x)] + list(split_constant(plan.x_forward(size_x)))
    tables += [tripled_constant(matrix) for matrix in plan.jump_sources()]
    tables += list(split_constant(plan.x_backward(size_x)) + split_constant(plan.jumps()))
    tables += [plan.symbol_tables(long)] + list(split_constant(plan.x_forward(long)))
    tables += list(split_constant(plan.x_backward(long)) + split_constant(plan.ends()))
    tables += [tripled_constant(matrix) for matrix in plan.end_sources()]
    half, pairs = size_x // 2, steps // 2

    def held(*shape):
        return pltpu.VMEM(shape, jnp.float32)

    halves, parts = (each, 2 * half, size_y), (pairs, each, 2 * own, size_y)
    both = (each, 2, 2 * half, size_y)
    slots = (slabs, each, sent_rows, size_y)
    spectrum = pl.pallas_call(
        functools.partial(spread, plan),
        name="spread",
        in_specs=[scalars, scalars, anywhere]
        + [pl.BlockSpec(memory_space=pltpu.VMEM) for table in tables],
        out_specs=anywhere,
        out_shape=shaped(*by_plane),
        scratch_shapes=[
            held(padded, 2, blocks, 4, block, size_y),
            held(*slots),
            held(*slots),
            held(*halves),
            held(*both),
            held(*halves),
            held(*parts),
            held(*parts),
            held(*parts),
            held(*parts),
            held(*halves),
            held(*both),
            held(*slots),
            held(*slots),
        ]
        + [pltpu.SemaphoreType.DMA((2, each))] * 6
        + [pltpu.SemaphoreType.DMA((padded,))] * 2,
        compiler_params=pltpu.CompilerParams(
            collective_id=0, has_side_effects=True, vmem_limit_bytes=56 * 1024 * 1024
        ),
    )(floats, wave_z, spectrum.reshape(by_plane), *tables)

    z_backward = plan.z_backward()
    most = min(256, 2 * rows)
    z_tables = split_constant(z_backward[:, :most])
    rest = z_backward[:, most:] if most < 2 * rows else z_backward[:, :16]
    tables = list(split_constant(plan.y_backward()) + z_tables) + [tripled_constant(rest)]
    result = called(
        functools.partial(leave_kernel, plan),
        "leave",
        (blocks,),
        [
            scalars,
            pl.BlockSpec((2, 1, rows * block, size_y), lambda at: (0, at, 0, 0)),
            pl.BlockSpec((1, block, size_z, size_y), lambda at: (3, at, 0, 0)),
        ]
        + [whole(table) for table in tables],
        pl.BlockSpec((4, block, size_z, size_y), lambda at: (0, at, 0, 0)),
        shaped(4, long, size_z, size_y),
        [
            floats,
            spectrum.reshape(2, blocks, rows * block, size_y),
            iterate,
        ]
        + tables,
    )
    return result[None]


def solution(mesh):
    placed = (
        P("tm", None, "space", None, None),
        P("tm", None, "space", None, None),
        P("space", None, None),
        P(),
    )
    return jax.shard_map(
        shards,
        mesh=mesh,
        in_specs=placed,
        out_specs=P("tm", None, "space", None, None),
        check_vma=False,
    )
```

```python
import functools
import math

import jax
import jax.numpy as jnp
import numpy as np
from jax import lax
from jax.experimental import pallas as pl
from jax.experimental.pallas import tpu as pltpu
from jax.sharding import PartitionSpec as P

diffusion_number = 16.0
circulant_alpha = 0.1
MESH = pl.DeviceIdType.MESH


def collocation_matrix():
    radau_nodes = [0.08858795951270394, 0.4094668644407347, 0.7876594617608471, 1.0]
    matrix = [[0.0] * 4 for row_index in range(4)]
    for column_index in range(4):
        coefficients = [1.0]
        for other_index in range(4):
            if other_index != column_index:
                scale_value = 1.0 / (radau_nodes[column_index] - radau_nodes[other_index])
                shifted = [0.0] + [value * scale_value for value in coefficients]
                lowered = [
                    -radau_nodes[other_index] * scale_value * value for value in coefficients
                ] + [0.0]
                coefficients = [
                    left_value + right_value for left_value, right_value in zip(shifted, lowered)
                ]
        for row_index in range(4):
            total = 0.0
            for power_index in range(len(coefficients)):
                total = total + coefficients[power_index] * radau_nodes[row_index] ** (
                    power_index + 1
                ) / (power_index + 1)
            matrix[row_index][column_index] = total
    return matrix


def solve_system(matrix, target):
    count = len(target)
    rows_list = [list(matrix[row_index]) + [target[row_index]] for row_index in range(count)]
    for column in range(count):
        best_row = column
        for candidate in range(column + 1, count):
            if abs(rows_list[candidate][column]) > abs(rows_list[best_row][column]):
                best_row = candidate
        saved_row = rows_list[column]
        rows_list[column] = rows_list[best_row]
        rows_list[best_row] = saved_row
        leader = rows_list[column][column]
        for other_row in range(count):
            if other_row != column:
                factor = rows_list[other_row][column] / leader
                rows_list[other_row] = [
                    left_value - factor * right_value
                    for left_value, right_value in zip(rows_list[other_row], rows_list[column])
                ]
    return [
        rows_list[row_index][count] / rows_list[row_index][row_index] for row_index in range(count)
    ]


def node_basis():
    matrix = collocation_matrix()
    helper = [[0.0] * 4 for row_index in range(4)]
    coefficients = [0.0, 0.0, 0.0, 0.0, 1.0]
    for order in range(1, 5):
        product = [
            [
                sum((matrix[row_index][inner] * helper[inner][column] for inner in range(4)))
                for column in range(4)
            ]
            for row_index in range(4)
        ]
        for row_index in range(4):
            product[row_index][row_index] = product[row_index][row_index] + coefficients[5 - order]
        helper = product
        trace_value = sum(
            (
                sum((matrix[row_index][inner] * helper[inner][row_index] for inner in range(4)))
                for row_index in range(4)
            )
        )
        coefficients[4 - order] = -trace_value / order
    roots_list = [(0.4 + 0.9j) ** power_index for power_index in range(4)]
    for sweep in range(400):
        for root_index in range(4):
            current = roots_list[root_index]
            numer = 0.0
            for power_index in range(4, -1, -1):
                numer = numer * current + coefficients[power_index]
            denom = 1.0
            for other_index in range(4):
                if other_index != root_index:
                    denom = denom * (current - roots_list[other_index])
            roots_list[root_index] = current - numer / denom
    vectors = [[0.0] * 4 for row_index in range(4)]
    for root_index in range(4):
        shifted = [
            [
                matrix[row_index][column] - (roots_list[root_index] if row_index == column else 0.0)
                for column in range(3)
            ]
            for row_index in range(3)
        ]
        target = [-matrix[row_index][3] for row_index in range(3)]
        parts = solve_system(shifted, target) + [1.0 + 0j]
        for row_index in range(4):
            vectors[row_index][root_index] = parts[row_index]
    inverse = [[0.0] * 4 for row_index in range(4)]
    for column in range(4):
        unit = [1.0 if row_index == column else 0.0 for row_index in range(4)]
        parts = solve_system(vectors, unit)
        for row_index in range(4):
            inverse[row_index][column] = parts[row_index]
    weights = [sum((inverse[row_index][column] for column in range(4))) for row_index in range(4)]
    return (roots_list, vectors, inverse, weights)


def split_constant(matrix):
    high = matrix.astype(jnp.bfloat16)
    low = (matrix - high.astype(np.float64)).astype(jnp.bfloat16)
    return high, low


def split(value):
    high = value.astype(jnp.bfloat16)
    low = (value - high.astype(jnp.float32)).astype(jnp.bfloat16)
    return high, low


def dot(left, right):
    return jnp.dot(left, right, preferred_element_type=jnp.float32)


def table_times(high, low, value):
    value_high, value_low = split(value)
    if high.shape[1] <= 128 and value.shape[0] % 16 == 0:
        twice = jnp.concatenate((high, high), axis=1)
        both = jnp.concatenate((value_high, value_low), axis=0)
        return dot(twice, both) + dot(low, value_high)
    return dot(high, value_high) + dot(high, value_low) + dot(low, value_high)


def times_table(value, high, low):
    value_high, value_low = split(value)
    return dot(value_high, high) + dot(value_low, high) + dot(value_high, low)


def tripled(value):
    high = value.astype(jnp.bfloat16).astype(jnp.float32)
    return jnp.concatenate((high, value - high, high), axis=0).astype(jnp.bfloat16)


def tripled_constant(matrix):
    high, low = split_constant(matrix)
    return np.concatenate((high, high, low), axis=1)


def complex_block(matrix):
    return np.block([[matrix.real, -matrix.imag], [matrix.imag, matrix.real]])


def fourier(rows, columns, length, sign):
    phases = np.outer(rows, columns) % length
    return np.exp(sign * 2j * np.pi * phases / length)


class Plan:
    def __init__(self, slabs, steps, size_x, size_z, size_y):
        self.slabs, self.steps = slabs, steps
        self.size_x, self.size_z, self.size_y = size_x, size_z, size_y
        self.long = long = size_x // slabs
        self.planes = size_z // 2 + 1
        each = -(-self.planes // slabs)
        while (each * slabs) % 2:
            each += 1
        self.each = each
        self.padded = each * slabs
        self.rows = 4 * self.padded
        self.block = 8
        self.blocks = long // self.block
        self.own_x = size_x // steps
        self.sent = 2 * long + 16
        self.values, self.vectors, self.inverse, self.weights = node_basis()
        self.matrix = np.array(collocation_matrix())

    def symbol_tables(self, length):
        theta_x = 2.0 * np.pi * np.arange(length)[:, None] / length
        theta_y = 2.0 * np.pi * np.arange(self.size_y)[None, :] / self.size_y
        real = diffusion_number * (2.0 * np.cos(theta_x) + 2.0 * np.cos(theta_y) - 4.0)
        ones = np.ones_like(real)
        return np.stack((real, np.sin(theta_x) * ones, np.sin(theta_y) * ones)).astype(np.float32)

    def z_symbols(self):
        theta = 2.0 * np.pi * np.arange(self.padded) / self.size_z
        return np.stack((diffusion_number * (2.0 * np.cos(theta) - 2.0), np.sin(theta))).astype(
            np.float32
        )

    def z_forward(self):
        wave = fourier(np.arange(self.padded), np.arange(self.size_z), self.size_z, -1.0)
        wave[self.planes :] = 0.0
        full = np.einsum("mn,kz->mknz", np.array(self.inverse), wave)
        full = full.reshape(self.rows, 4 * self.size_z)
        return np.concatenate((full.real, full.imag), axis=0)

    def z_backward(self):
        wave = fourier(np.arange(self.size_z), np.arange(self.padded), self.size_z, 1.0)
        weight = np.full(self.padded, 2.0)
        weight[0] = 1.0
        weight[self.planes - 1] = 1.0
        weight[self.planes :] = 0.0
        wave = wave * weight / self.size_z
        full = np.einsum("nm,zk->nzmk", np.array(self.vectors), wave)
        full = full.reshape(4 * self.size_z, self.rows)
        return np.concatenate((full.real, -full.imag), axis=1)

    def y_forward(self):
        span = np.arange(self.size_y)
        return complex_block(fourier(span, span, self.size_y, -1.0)).T

    def y_backward(self):
        span = np.arange(self.size_y)
        return complex_block(fourier(span, span, self.size_y, 1.0)).T / self.size_y

    def x_forward(self, length):
        span = np.arange(length)
        return complex_block(fourier(span, span, length, -1.0))

    def x_backward(self, length):
        span = np.arange(length)
        return complex_block(fourier(span, span, length, 1.0)) / length

    def ends(self):
        points = np.array([0, self.long - 1])
        wave = fourier(points, np.arange(self.long), self.long, 1.0) / self.long
        full = complex_block(wave)[[0, 2, 1, 3]]
        return np.concatenate((full, full, full, full), axis=0)

    def jump_sources(self):
        wave = np.arange(self.size_x)
        even = []
        for slab in range(self.slabs):
            start = slab * self.long

            def phase(point):
                return fourier(wave, np.array([point % self.size_x]), self.size_x, -1.0)[:, 0]

            first = phase(start - 1) - phase(start + self.long - 1)
            last = phase(start + self.long) - phase(start)
            even.append(np.stack((first, 1j * first, last, 1j * last), axis=1))
        return self.by_parity(even)

    def by_parity(self, blocks):
        zero = np.zeros_like(blocks[0])
        even = np.concatenate([part for block in blocks for part in (block, zero)], axis=1)
        odd = np.concatenate([part for block in blocks for part in (zero, block)], axis=1)
        return [np.concatenate((full.real, full.imag), axis=0) for full in (even, odd)]

    def end_sources(self):
        wave = np.arange(self.long)
        upper = fourier(wave, np.array([1]), self.long, 1.0)[:, 0]
        lower = np.ones_like(upper)
        return self.by_parity([np.stack((upper, 1j * upper, lower, 1j * lower), axis=1)])

    def jumps(self):
        wave = np.arange(self.size_x)
        rows = []
        for slab in range(self.slabs):
            start = slab * self.long
            points = np.array([start + self.long, start, start - 1, start + self.long - 1])
            value = fourier(points % self.size_x, wave, self.size_x, 1.0) / self.size_x
            upper, lower = value[0] - value[1], value[2] - value[3]
            full = complex_block(np.stack((upper, lower)))[[0, 2, 1, 3]]
            rows += [full, full]
        return np.concatenate(rows, axis=0)


def damped_by(real, imag, value):
    lower_real = 1.0 - (real * value.real - imag * value.imag)
    lower_imag = real * value.imag + imag * value.real
    scale = 1.0 / (lower_real * lower_real + lower_imag * lower_imag)
    return lower_real * scale, lower_imag * scale


def symbol(table, floats, wave_z, plane):
    real = table[0] + wave_z[0, plane]
    imag = -(floats[0] * table[1] + floats[1] * table[2] + floats[2] * wave_z[1, plane])
    return real, imag


def times(left, right):
    return (left[0] * right[0] - left[1] * right[1], left[0] * right[1] + left[1] * right[0])


def plus(left, right):
    return (left[0] + right[0], left[1] + right[1])


def number(value):
    value = complex(value)
    return (value.real, value.imag)


def end_scale(floats, shape):
    row = lax.broadcasted_iota(jnp.int32, shape, 0) % 4
    upper = diffusion_number - 0.5 * floats[0]
    lower = diffusion_number + 0.5 * floats[0]
    return jnp.where(row < 2, upper, lower)


def enter_kernel(plan, floats, it, below, above, right, diff, field, *refs):
    z_high, z_low, y_high, y_low, out, buffer, halo, sends, receives = refs
    block, rows, size_y, slabs = plan.block, plan.rows, plan.size_y, plan.slabs
    count = plan.blocks
    turn = pl.program_id(0)
    at = (turn + 1) % count
    step, slab = lax.axis_index("tm"), lax.axis_index("space")
    upper_slab, lower_slab = (step, (slab + 1) % slabs), (step, (slab + slabs - 1) % slabs)

    def edge(index):
        plane = (plan.long - 1, 0)[index]
        return pltpu.make_async_remote_copy(
            src_ref=field.at[:, pl.ds(plane, 1)],
            dst_ref=halo.at[index],
            send_sem=sends.at[index],
            recv_sem=receives.at[index],
            device_id=(upper_slab, lower_slab)[index],
            device_id_type=MESH,
        )

    @pl.when(turn == 0)
    def _():
        barrier = pltpu.get_barrier_semaphore()
        for device in (upper_slab, lower_slab):
            pl.semaphore_signal(barrier, inc=1, device_id=device, device_id_type=MESH)
        pl.semaphore_wait(barrier, 2)
        for index in range(2):
            edge(index).start()

    @pl.when(turn == max(count - 2, 0))
    def _():
        for index in range(2):
            edge(index).wait()

    buffer[:, 1 : block + 1] = it[...]
    buffer[:, 0:1] = below[...]
    buffer[:, block + 1 :] = above[...]

    @pl.when(at == 0)
    def _():
        buffer[:, 0:1] = halo[0]

    @pl.when(at == count - 1)
    def _():
        buffer[:, block + 1 :] = halo[1]

    is_last = (step == plan.steps - 1).astype(jnp.float32)
    nodes = plan.matrix.sum(axis=1)
    size_z = plan.size_z

    def driving(plane):
        factor = diffusion_number * (diff[plane] - 1.0)
        terms = []
        for node in range(4):
            center = buffer[node, plane + 1]
            upper, lower = buffer[node, plane + 2], buffer[node, plane]
            z_up, z_down = pltpu.roll(center, size_z - 1, 0), pltpu.roll(center, 1, 0)
            y_up, y_down = pltpu.roll(center, size_y - 1, 1), pltpu.roll(center, 1, 1)
            laplace = (upper + lower) + (z_up + z_down) + (y_up + y_down) - 6.0 * center
            terms.append(factor * laplace)
        transport = (
            floats[0] * (upper - lower) + floats[1] * (y_up - y_down) + floats[2] * (z_up - z_down)
        )
        operated = is_last * (diffusion_number * laplace - 0.5 * transport)
        kept = is_last * center
        result = []
        for row in range(4):
            total = right[row, plane] + (float(nodes[row]) * operated - kept)
            for column in range(4):
                total = total + float(plan.matrix[row, column]) * terms[column]
            result.append(total)
        return jnp.concatenate(result, axis=0)

    def pair(index, carry):
        plane = 2 * index
        both = jnp.concatenate((driving(plane), driving(plane + 1)), axis=1)
        along_z = table_times(z_high[...], z_low[...], both)
        real, imag = along_z[:rows], along_z[rows:]
        stacked = jnp.concatenate(
            (
                jnp.concatenate((real[:, :size_y], imag[:, :size_y]), axis=1),
                jnp.concatenate((real[:, size_y:], imag[:, size_y:]), axis=1),
            ),
            axis=0,
        )
        along_y = times_table(stacked, y_high[...], y_low[...])
        for offset in range(2):
            part = along_y[offset * rows : (offset + 1) * rows]
            where = pl.ds(plane + offset, rows, stride=block)
            out[0, 0, where, :] = part[:, :size_y]
            out[1, 0, where, :] = part[:, size_y:]
        return carry

    lax.fori_loop(0, block // 2, pair, 0, unroll=4)


def end_spectra(plan, floats, tiles, even, odd):
    size_x, size_y = plan.size_x, plan.size_y
    pairs = []
    for pair in range(2):
        rows = jnp.concatenate([tiles[slab][8 * pair : 8 * pair + 8] for slab in range(plan.slabs)])
        pairs.append(rows * end_scale(floats, rows.shape))
    value = tripled(jnp.concatenate(pairs, axis=1))
    found = [dot(even[...], value), dot(odd[...], value)]
    result = []
    for mode in range(4):
        lanes = slice((mode // 2) * size_y, (mode // 2 + 1) * size_y)
        part = found[mode % 2][:, lanes]
        result.append(times(number(plan.values[mode]), (part[:size_x], part[size_x:])))
    return result


def spread(plan, floats, wave_z, *refs):
    (given, table, f_high, f_low, even, odd, b_high, b_low, j_high, j_low) = refs[:10]
    (local, lf_high, lf_low, lb_high, lb_low, e_high, e_low, end_even, end_odd, out) = refs[10:20]
    (held, sent, x_in, f_send, f_all, growth, c_send, c_all, s_send) = refs[20:29]
    (s_all, d_send, d_all, x_out, y_in) = refs[29:34]
    (x_sems, f_sems, c_sems, s_sems, d_sems, y_sems, in_sems, out_sems) = refs[34:]
    slabs, steps, each = plan.slabs, plan.steps, plan.each
    long, size_x, size_y, own = plan.long, plan.size_x, plan.size_y, plan.own_x
    half, pairs = size_x // 2, steps // 2
    step, slab = lax.axis_index("tm"), lax.axis_index("space")
    parity, place = step % 2, step // 2
    other = (step + 1 - 2 * parity, slab)

    def peer(index):
        return (2 * index + parity, slab)

    def slab_peer(index):
        return (step, index)

    barrier = pltpu.get_barrier_semaphore()
    neighbours = [other]
    neighbours += [slab_peer((slab + shift) % slabs) for shift in range(1, slabs)]
    neighbours += [peer((place + shift) % pairs) for shift in range(1, pairs)]
    for device in neighbours:
        pl.semaphore_signal(barrier, inc=1, device_id=device, device_id_type=MESH)
    pl.semaphore_wait(barrier, len(neighbours))

    def remote(source, target, sems, plane, device):
        return pltpu.make_async_remote_copy(
            src_ref=source,
            dst_ref=target,
            send_sem=sems.at[0, plane],
            recv_sem=sems.at[1, plane],
            device_id=device,
            device_id_type=MESH,
        )

    def await_all(ref, sems, kind, plane):
        pltpu.make_async_copy(ref, ref, sems.at[kind, plane]).wait()

    def fetch(plane):
        return pltpu.make_async_copy(given.at[:, :, :, plane], held.at[plane], in_sems.at[plane])

    def write(plane):
        return pltpu.make_async_copy(held.at[plane], out.at[:, :, :, plane], out_sems.at[plane])

    def fetch_all(plane, carry):
        for index in range(slabs):
            fetch(index * each + plane).start()
        return carry

    lax.fori_loop(0, each, fetch_all, 0)

    def local_mode(index):
        return slice(index * size_y, (index + 1) * size_y)

    def spectrum_of(plane, index):
        at = index * each + plane
        parts = [
            jnp.concatenate(
                [held[at, part, :, mode].reshape(long, size_y) for mode in range(4)], axis=1
            )
            for part in range(2)
        ]
        return table_times(lf_high[...], lf_low[...], jnp.concatenate(parts, axis=0))

    def modes_of(plane, index, spectrum):
        at = index * each + plane
        a_real, a_imag = symbol(local, floats, wave_z, at)
        total, inner = None, []
        shape = (plan.blocks, plan.block, size_y)
        for mode in range(4):
            part = (spectrum[:long, local_mode(mode)], spectrum[long:, local_mode(mode)])
            held[at, 0, :, mode] = part[0].reshape(shape)
            held[at, 1, :, mode] = part[1].reshape(shape)
            part = times(damped_by(a_real, a_imag, complex(plan.values[mode])), part)
            total = part if total is None else plus(total, part)
            inner.append(jnp.concatenate(part, axis=0))
        sent[index, plane, : 2 * long] = table_times(
            lb_high[...], lb_low[...], jnp.concatenate(total, axis=0)
        )
        ends = table_times(e_high[...], e_low[...], jnp.concatenate(inner, axis=1))[:8]
        upper = lax.broadcasted_iota(jnp.int32, (8, size_y), 0) < 4
        for pair in range(2):
            start = 2 * long + 8 * pair
            sent[index, plane, start : start + 8] = jnp.where(
                upper, ends[:, local_mode(2 * pair)], ends[:, local_mode(2 * pair + 1)]
            )

    def modes_stage(plane):
        targets = [(slab + shift) % slabs for shift in range(1, slabs)]
        for index in range(slabs):
            fetch(index * each + plane).wait()
        spectra = [spectrum_of(plane, index) for index in range(slabs)]
        for index in range(slabs):
            modes_of(plane, index, spectra[index])
        x_in[slab, plane] = sent[slab, plane]
        for target in targets:
            remote(
                sent.at[target, plane], x_in.at[slab, plane], x_sems, plane, slab_peer(target)
            ).start()

    def solution_of(plane, index):
        at = index * each + plane
        found = table_times(lf_high[...], lf_low[...], y_in[index, plane, : 2 * long])
        before = (found[:long], found[long:])
        start = 2 * long
        ends = jnp.concatenate(
            (y_in[index, plane, start : start + 8], y_in[index, plane, start + 8 :]), axis=1
        )
        value = tripled(ends * end_scale(floats, ends.shape))
        sources = [dot(end_even[...], value), dot(end_odd[...], value)]
        a_real, a_imag = symbol(local, floats, wave_z, at)
        driven = []
        for mode in range(4):
            source = sources[mode % 2][:, local_mode(mode // 2)]
            total = times(number(plan.values[mode]), (source[:long], source[long:]))
            total = plus(total, times(number(plan.weights[mode]), before))
            kept = [held[at, part, :, mode].reshape(long, size_y) for part in range(2)]
            total = plus(total, kept)
            damped = damped_by(a_real, a_imag, complex(plan.values[mode]))
            driven.append(jnp.concatenate(times(damped, total), axis=0))
        return jnp.concatenate(driven, axis=1)

    def keep_solution(plane, index, driven):
        at = index * each + plane
        back = table_times(lb_high[...], lb_low[...], driven)
        shape = (plan.blocks, plan.block, size_y)
        for mode in range(4):
            held[at, 0, :, mode] = back[:long, local_mode(mode)].reshape(shape)
            held[at, 1, :, mode] = back[long:, local_mode(mode)].reshape(shape)

    def solution_stage(plane):
        if slabs > 1:
            await_all(x_out.at[pl.ds(0, slabs - 1), plane], y_sems, 1, plane)
        driven = [solution_of(plane, index) for index in range(slabs)]
        for index in range(slabs):
            keep_solution(plane, index, driven[index])
        for index in range(slabs):
            write(index * each + plane).start()

    def symbols(plane, start, count):
        rows = pl.ds(start, count)
        tables = [table[index, rows] for index in range(3)]
        return symbol(tables, floats, wave_z, slab * each + plane)

    def grown(plane, start, count):
        a_real, a_imag = symbols(plane, start, count)
        total = None
        for mode in range(4):
            damped = damped_by(a_real, a_imag, complex(plan.values[mode]))
            term = times(number(plan.weights[mode]), damped)
            total = term if total is None else plus(total, term)
        return total

    def spectrum_stage(plane):
        if slabs > 1:
            await_all(x_in.at[pl.ds(0, slabs - 1), plane], x_sems, 1, plane)
        arrived = [x_in[index, plane] for index in range(slabs)]
        value = jnp.concatenate(
            [part[:long] for part in arrived] + [part[long : 2 * long] for part in arrived], axis=0
        )
        found = table_times(f_high[...], f_low[...], value)
        total = (found[:size_x], found[size_x:])
        sources = end_spectra(plan, floats, [part[2 * long :] for part in arrived], even, odd)
        a_real, a_imag = symbols(plane, 0, size_x)
        for mode in range(4):
            damped = damped_by(a_real, a_imag, complex(plan.values[mode]))
            total = plus(total, times(damped, sources[mode]))
        for index in range(2):
            rows = slice(index * half, (index + 1) * half)
            lower, upper = total[index][:half], total[index][half:]
            f_send[plane, rows] = jnp.where(parity == 0, upper, lower)
            f_all[plane, parity, rows] = jnp.where(parity == 0, lower, upper)
        remote(f_send.at[plane], f_all.at[plane, parity], f_sems, plane, other).start()

    def pair_stage(plane):
        factor = grown(plane, pl.multiple_of(parity * half, half), half)
        growth[plane, :half], growth[plane, half:] = factor
        await_all(f_send.at[plane], f_sems, 1, plane)
        early = (f_all[plane, 0, :half], f_all[plane, 0, half:])
        later = (f_all[plane, 1, :half], f_all[plane, 1, half:])
        total = plus(later, times(factor, early))
        for index in range(pairs):
            rows = slice(index * own, (index + 1) * own)
            c_send[index, plane, :own] = total[0][rows]
            c_send[index, plane, own:] = total[1][rows]
        c_all[place, plane] = c_send[place, plane]
        for shift in range(1, pairs):
            target = (place + shift) % pairs
            remote(
                c_send.at[target, plane], c_all.at[place, plane], c_sems, plane, peer(target)
            ).start()

    def sweep_stage(plane):
        factor = grown(plane, pl.multiple_of(parity * half + place * own, own), own)
        factor = times(factor, factor)
        if pairs > 1:
            await_all(c_all.at[pl.ds(0, pairs - 1), plane], c_sems, 1, plane)
        fields = [(c_all[index, plane, :own], c_all[index, plane, own:]) for index in range(pairs)]
        total, power = fields[0], factor
        for index in range(1, pairs):
            total = plus(fields[index], times(factor, total))
            power = times(factor, power)
        lower = (1.0 - circulant_alpha * power[0], -circulant_alpha * power[1])
        scale = circulant_alpha / (lower[0] * lower[0] + lower[1] * lower[1])
        current = times(total, (lower[0] * scale, -lower[1] * scale))
        for index in range(pairs):
            s_send[index, plane, :own] = current[0]
            s_send[index, plane, own:] = current[1]
            current = plus(fields[index], times(factor, current))
        s_all[place, plane] = s_send[place, plane]
        for shift in range(1, pairs):
            target = (place + shift) % pairs
            remote(
                s_send.at[target, plane], s_all.at[place, plane], s_sems, plane, peer(target)
            ).start()

    def start_stage(plane):
        if pairs > 1:
            await_all(s_all.at[pl.ds(0, pairs - 1), plane], s_sems, 1, plane)
        early = tuple(
            jnp.concatenate([s_all[index, plane, rows] for index in range(pairs)], axis=0)
            for rows in (slice(0, own), slice(own, 2 * own))
        )
        field = (f_all[plane, 0, :half], f_all[plane, 0, half:])
        later = plus(field, times((growth[plane, :half], growth[plane, half:]), early))
        for index in range(2):
            rows = slice(index * half, (index + 1) * half)
            d_send[plane, rows] = jnp.where(parity == 0, later[index], early[index])
            d_all[plane, parity, rows] = jnp.where(parity == 0, early[index], later[index])
        remote(d_send.at[plane], d_all.at[plane, parity], d_sems, plane, other).start()

    def return_stage(plane):
        await_all(d_send.at[plane], d_sems, 1, plane)
        real = jnp.concatenate((d_all[plane, 0, :half], d_all[plane, 1, :half]), axis=0)
        imag = jnp.concatenate((d_all[plane, 0, half:], d_all[plane, 1, half:]), axis=0)
        found = table_times(b_high[...], b_low[...], jnp.concatenate((real, imag), axis=0))
        tiles = [x_in[index, plane, 2 * long :] for index in range(slabs)]
        sources = end_spectra(plan, floats, tiles, even, odd)
        a_real, a_imag = symbols(plane, 0, size_x)
        driven = []
        for mode in range(4):
            damped = damped_by(a_real, a_imag, complex(plan.values[mode]))
            weighted = times(number(plan.weights[mode]), (real, imag))
            driven.append(jnp.concatenate(times(damped, plus(weighted, sources[mode])), axis=0))
        jumps = table_times(j_high[...], j_low[...], jnp.concatenate(driven, axis=1))
        row = lax.broadcasted_iota(jnp.int32, (8, size_y), 0)
        for index in range(slabs):
            first = index * long
            x_out[index, plane, :long] = found[first : first + long]
            x_out[index, plane, long : 2 * long] = found[size_x + first : size_x + first + long]
            above, under = tiles[(index + 1) % slabs], tiles[(index - 1) % slabs]
            for pair in range(2):
                part = slice(8 * pair, 8 * pair + 8)
                here = slice(8 * index, 8 * index + 8)
                local = jnp.where(row % 4 < 2, above[part], under[part]) - tiles[index][part]
                lower = jumps[here, 2 * pair * size_y : (2 * pair + 1) * size_y]
                upper = jumps[here, (2 * pair + 1) * size_y : (2 * pair + 2) * size_y]
                start = 2 * long + 8 * pair
                x_out[index, plane, start : start + 8] = local + jnp.where(row < 4, lower, upper)
        y_in[slab, plane] = x_out[slab, plane]
        for shift in range(1, slabs):
            target = (slab + shift) % slabs
            remote(
                x_out.at[target, plane], y_in.at[slab, plane], y_sems, plane, slab_peer(target)
            ).start()

    stages = (modes_stage, spectrum_stage, pair_stage, sweep_stage)
    stages += (start_stage, return_stage, solution_stage)

    delays = (0, 1, 2, 4, 6, 7, 8)

    def iteration(time, carry):
        for delay in range(len(stages)):
            plane = time - delays[delay]

            @pl.when(jnp.logical_and(plane >= 0, plane < each))
            def _():
                stages[delay](plane)

        return carry

    lax.fori_loop(0, each + delays[-1], iteration, 0)

    def finish(plane, carry):
        await_all(f_send.at[plane], f_sems, 0, plane)
        await_all(d_send.at[plane], d_sems, 0, plane)
        if pairs > 1:
            await_all(c_send.at[pl.ds(0, pairs - 1), plane], c_sems, 0, plane)
            await_all(s_send.at[pl.ds(0, pairs - 1), plane], s_sems, 0, plane)
        if slabs > 1:
            await_all(x_in.at[pl.ds(0, slabs - 1), plane], x_sems, 0, plane)
            await_all(x_out.at[pl.ds(0, slabs - 1), plane], y_sems, 0, plane)
        for index in range(slabs):
            write(index * each + plane).wait()
        return carry

    lax.fori_loop(0, each, finish, 0)


def leave_kernel(plan, found_in, kept, y_high, y_low, z_high, z_low, z_rest, out):
    block, rows, size_y, size_z = plan.block, plan.rows, plan.size_y, plan.size_z
    most = z_high.shape[1]
    is_last = (lax.axis_index("tm") == plan.steps - 1).astype(jnp.float32)

    def pair(index, carry):
        plane = 2 * index
        parts = []
        for offset in range(2):
            where = pl.ds(plane + offset, rows, stride=block)
            parts.append(jnp.concatenate((found_in[0, 0, where, :], found_in[1, 0, where, :]), axis=1))
        along_y = times_table(jnp.concatenate(parts, axis=0), y_high[...], y_low[...])
        stacked = jnp.concatenate(
            (
                jnp.concatenate((along_y[:rows, :size_y], along_y[rows:, :size_y]), axis=1),
                jnp.concatenate((along_y[:rows, size_y:], along_y[rows:, size_y:]), axis=1),
            ),
            axis=0,
        )
        found = table_times(z_high[...], z_low[...], stacked[:most])
        if most < 2 * rows:
            found = found + dot(z_rest[...], tripled(stacked[most:]))
        for offset in range(2):
            add = is_last * kept[0, plane + offset]
            for node in range(4):
                part = found[node * size_z : (node + 1) * size_z]
                out[node, plane + offset] = part[:, offset * size_y : (offset + 1) * size_y] + add
        return carry

    lax.fori_loop(0, block // 2, pair, 0, unroll=4)


def whole(array):
    zeros = (0,) * array.ndim
    return pl.BlockSpec(array.shape, lambda *at: zeros)


scalars = pl.BlockSpec(memory_space=pltpu.SMEM)


def called(kernel, name, grid, in_specs, out_specs, out_shape, operands, scratch=(), collective=None):
    return pl.pallas_call(
        kernel,
        name=name,
        grid=grid,
        in_specs=in_specs,
        out_specs=out_specs,
        out_shape=out_shape,
        scratch_shapes=list(scratch),
        compiler_params=pltpu.CompilerParams(
            dimension_semantics=("arbitrary",) * len(grid),
            vmem_limit_bytes=56 * 1024 * 1024,
            collective_id=collective,
            has_side_effects=collective is not None,
        ),
    )(*operands)


def shaped(*shape):
    return jax.ShapeDtypeStruct(shape, jnp.float32)


def shards(iterate, right_side, diffusivity, velocity):
    steps = lax.axis_size("tm")
    slabs = lax.axis_size("space")
    nodes, long, size_z, size_y = iterate.shape[1:]
    plan = Plan(slabs, steps, long * slabs, size_z, size_y)
    size_x, padded, each = plan.size_x, plan.padded, plan.each
    rows, block, blocks, sent_rows, own = plan.rows, plan.block, plan.blocks, plan.sent, plan.own_x
    iterate, right_side = iterate[0], right_side[0]

    floats = velocity
    wave_z = jnp.asarray(plan.z_symbols())

    z_tables = split_constant(plan.z_forward())
    y_tables = split_constant(plan.y_forward())
    tables = list(z_tables + y_tables)
    thin = (4, 1, size_z, size_y)
    anywhere = pl.BlockSpec(memory_space=pl.ANY)

    def turned(at):
        return (at + 1) % blocks

    spectrum = called(
        functools.partial(enter_kernel, plan),
        "enter",
        (blocks,),
        [
            scalars,
            pl.BlockSpec((4, block, size_z, size_y), lambda at: (0, turned(at), 0, 0)),
            pl.BlockSpec(thin, lambda at: (0, jnp.maximum(turned(at) * block - 1, 0), 0, 0)),
            pl.BlockSpec(
                thin, lambda at: (0, jnp.minimum(turned(at) * block + block, long - 1), 0, 0)
            ),
            pl.BlockSpec((4, block, size_z, size_y), lambda at: (0, turned(at), 0, 0)),
            pl.BlockSpec((block, size_z, size_y), lambda at: (turned(at), 0, 0)),
            anywhere,
        ]
        + [whole(table) for table in tables],
        pl.BlockSpec((2, 1, rows * block, size_y), lambda at: (0, turned(at), 0, 0)),
        shaped(2, blocks, rows * block, size_y),
        [floats, iterate, iterate, iterate, right_side, diffusivity, iterate] + tables,
        scratch=[
            pltpu.VMEM((4, block + 2, size_z, size_y), jnp.float32),
            pltpu.VMEM((2,) + thin, jnp.float32),
            pltpu.SemaphoreType.DMA((2,)),
            pltpu.SemaphoreType.DMA((2,)),
        ],
        collective=1,
    )

    by_plane = (2, blocks, 4, padded, block, size_y)
    tables = [plan.symbol_tables(size_x)] + list(split_constant(plan.x_forward(size_x)))
    tables += [tripled_constant(matrix) for matrix in plan.jump_sources()]
    tables += list(split_constant(plan.x_backward(size_x)) + split_constant(plan.jumps()))
    tables += [plan.symbol_tables(long)] + list(split_constant(plan.x_forward(long)))
    tables += list(split_constant(plan.x_backward(long)) + split_constant(plan.ends()))
    tables += [tripled_constant(matrix) for matrix in plan.end_sources()]
    half, pairs = size_x // 2, steps // 2

    def held(*shape):
        return pltpu.VMEM(shape, jnp.float32)

    halves, parts = (each, 2 * half, size_y), (pairs, each, 2 * own, size_y)
    both = (each, 2, 2 * half, size_y)
    slots = (slabs, each, sent_rows, size_y)
    spectrum = pl.pallas_call(
        functools.partial(spread, plan),
        name="spread",
        in_specs=[scalars, scalars, anywhere]
        + [pl.BlockSpec(memory_space=pltpu.VMEM) for table in tables],
        out_specs=anywhere,
        out_shape=shaped(*by_plane),
        scratch_shapes=[
            held(padded, 2, blocks, 4, block, size_y),
            held(*slots),
            held(*slots),
            held(*halves),
            held(*both),
            held(*halves),
            held(*parts),
            held(*parts),
            held(*parts),
            held(*parts),
            held(*halves),
            held(*both),
            held(*slots),
            held(*slots),
        ]
        + [pltpu.SemaphoreType.DMA((2, each))] * 6
        + [pltpu.SemaphoreType.DMA((padded,))] * 2,
        compiler_params=pltpu.CompilerParams(
            collective_id=0, has_side_effects=True, vmem_limit_bytes=56 * 1024 * 1024
        ),
    )(floats, wave_z, spectrum.reshape(by_plane), *tables)

    z_backward = plan.z_backward()
    most = min(256, 2 * rows)
    z_tables = split_constant(z_backward[:, :most])
    rest = z_backward[:, most:] if most < 2 * rows else z_backward[:, :16]
    tables = list(split_constant(plan.y_backward()) + z_tables) + [tripled_constant(rest)]
    result = called(
        functools.partial(leave_kernel, plan),
        "leave",
        (blocks,),
        [
            pl.BlockSpec((2, 1, rows * block, size_y), lambda at: (0, at, 0, 0)),
            pl.BlockSpec((1, block, size_z, size_y), lambda at: (3, at, 0, 0)),
        ]
        + [whole(table) for table in tables],
        pl.BlockSpec((4, block, size_z, size_y), lambda at: (0, at, 0, 0)),
        shaped(4, long, size_z, size_y),
        [
            spectrum.reshape(2, blocks, rows * block, size_y),
            iterate,
        ]
        + tables,
    )
    return result[None]


def solution(mesh):
    placed = (
        P("tm", None, "space", None, None),
        P("tm", None, "space", None, None),
        P("space", None, None),
        P(),
    )
    return jax.shard_map(
        shards,
        mesh=mesh,
        in_specs=placed,
        out_specs=P("tm", None, "space", None, None),
        check_vma=False,
    )
```
